32 devices in a mesh: row: 4 (over y, x), col: 8 (over z, core).
Axes of the slice: x: 2, y: 2, z: 4, core: 2. Of those that a mesh axis runs over, the one named last changes fastest.
Arguments:
- left_matrix: float32 [4096, 4096], P('row', 'col'), may hold values from -6 to 6
- right_matrix: float32 [4096, 4096], P('row', 'col'), may hold values from -0.09375 to 0.09375
Outputs:
- product_matrix: float32 [4096, 4096], P('row', 'col')
The draws below stay inside these ranges and needn't reach their ends.
All inputs are finite; a program needn't handle non-finite values.
Results may differ from the reference program's by a relative error of at most 0.00019.
Values sent between devices are 32-bit elements; how exact they have to be, the bound alone decides.
A program may use at most 64 MiB of HBM per device.

```python
import jax
import jax.numpy as jnp
from jax import lax

ORDER = 4096


def level_of(own_key, dims, split, least, high):
    def one(position, blocks):
        steps = jax.random.uniform(jax.random.fold_in(jax.random.fold_in(own_key, 6), position), (blocks,), jnp.float32, least / len(split), high / len(split))
        return jnp.repeat(jnp.exp(steps), dims[position] // blocks).reshape((-1,) + (1,) * (len(dims) - position - 1))

    gain = one(*split[0])
    for cut in split[1:]:
        gain = gain * one(*cut)
    return gain


def scatter_about(own_key, extent, spread, reach, split=(), dtype=jnp.bfloat16):
    gain = level_of(own_key, extent, split, -0.22, 0.18) if split else 1.0
    result = jax.random.normal(own_key, extent, jnp.float32) * spread * gain
    return jnp.minimum(jnp.maximum(result, -reach), reach).astype(dtype)


def setup_inputs(seed: int = 0) -> dict:
    arg_keys = jax.random.split(jax.random.key(seed), 3)
    left_matrix = scatter_about(arg_keys[0], (ORDER, ORDER), 1.0, 6.0, ((0, 4), (1, 8)), jnp.float32)
    right_matrix = scatter_about(arg_keys[1], (ORDER, ORDER), ORDER ** -0.5, 0.09375, ((0, 4), (1, 8)), jnp.float32)
    return {"left_matrix": left_matrix, "right_matrix": right_matrix}


def multiply(left_term, right_term):
    return jnp.dot(left_term, right_term, precision=lax.Precision.HIGHEST, preferred_element_type=jnp.float32)


def left_terms(upper_left, upper_right, lower_left, lower_right):
    sum_one = lower_left + lower_right
    sum_two = sum_one - upper_left
    sum_three = upper_left - lower_left
    sum_four = upper_right - sum_two
    return (upper_left, upper_right, sum_four, lower_right, sum_one, sum_two, sum_three)


def right_terms(upper_left, upper_right, lower_left, lower_right):
    diff_one = upper_right - upper_left
    diff_two = lower_right - diff_one
    diff_three = lower_right - upper_right
    diff_four = diff_two - lower_left
    return (upper_left, lower_left, lower_right, diff_four, diff_one, diff_two, diff_three)


def reference(left_matrix, right_matrix):
    half_order = ORDER // 2
    lefts = left_terms(left_matrix[:half_order, :half_order], left_matrix[:half_order, half_order:],
                       left_matrix[half_order:, :half_order], left_matrix[half_order:, half_order:])
    rights = right_terms(right_matrix[:half_order, :half_order], right_matrix[:half_order, half_order:],
                         right_matrix[half_order:, :half_order], right_matrix[half_order:, half_order:])
    products = [multiply(lefts[index], rights[index]) for index in range(7)]
    partial_two = products[0] + products[5]
    partial_three = partial_two + products[6]
    partial_four = partial_two + products[4]
    upper_left = products[0] + products[1]
    upper_right = partial_four + products[2]
    lower_left = partial_three - products[3]
    lower_right = partial_three + products[4]
    return jnp.block([[upper_left, upper_right], [lower_left, lower_right]])
```

```python
import functools

import jax
import jax.numpy as jnp
from jax import lax
from jax.experimental import pallas as pl
from jax.experimental.pallas import tpu as pltpu
from jax.sharding import PartitionSpec as P

MESH = pl.DeviceIdType.MESH
CHUNKS = 4


def split(value):
    high = value.astype(jnp.bfloat16)
    low = (value - high.astype(jnp.float32)).astype(jnp.bfloat16)
    return high, low


def kernel(rows, cols, a_in, b_in, out, a_all, b_all, b_high, b_low,
           a_recv, a_send, b_recv, b_send, local):
    row = lax.axis_index("row")
    col = lax.axis_index("col")
    core = lax.rem(col, 2)
    chip = lax.div(col, 2)
    chips = cols // 2
    height, a_depth = a_in.shape
    b_depth = b_in.shape[0]
    per_b = b_depth // a_depth
    size = height // CHUNKS
    partner = chip * 2 + 1 - core

    def left_valid(distance):
        return chip >= distance

    def right_valid(distance):
        return chip + distance < chips

    def a_copy(kind, block, chunk, own):
        part = pl.ds(chunk * size, size)
        target = (col + 2, col - 2, partner)[kind]
        return pltpu.make_async_remote_copy(
            src_ref=a_in.at[part] if own else a_all.at[block, part],
            dst_ref=a_all.at[block, part],
            send_sem=a_send.at[kind, block, chunk],
            recv_sem=a_recv.at[block, chunk],
            device_id={"col": target}, device_id_type=MESH)

    def a_wait(block, chunk):
        a_copy(2, block, chunk, False).wait_recv()

    def b_copy(peer, source):
        return pltpu.make_async_remote_copy(
            src_ref=b_in, dst_ref=b_all.at[source],
            send_sem=b_send.at[peer], recv_sem=b_recv.at[source],
            device_id={"row": peer}, device_id_type=MESH)

    barrier = pltpu.get_barrier_semaphore()

    @pl.when(chip > 0)
    def _():
        pl.semaphore_signal(barrier, inc=1, device_id={"col": col - 2}, device_id_type=MESH)

    @pl.when(chip < chips - 1)
    def _():
        pl.semaphore_signal(barrier, inc=1, device_id={"col": col + 2}, device_id_type=MESH)

    pl.semaphore_signal(barrier, inc=1, device_id={"col": partner}, device_id_type=MESH)
    peers = [lax.rem(row + offset, rows) for offset in range(1, rows)]
    for peer in peers:
        pl.semaphore_signal(barrier, inc=1, device_id={"row": peer}, device_id_type=MESH)
    own_a = pltpu.make_async_copy(a_in, a_all.at[col], local.at[0])
    own_b = pltpu.make_async_copy(b_in, b_all.at[row], local.at[1])
    own_a.start()
    own_b.start()
    near = jnp.where(chip > 0, 1, 0) + jnp.where(chip < chips - 1, 1, 0)
    pl.semaphore_wait(barrier, rows + near)

    for chunk in range(CHUNKS):
        @pl.when(right_valid(1))
        def _():
            a_copy(0, col, chunk, True).start()

        @pl.when(left_valid(1))
        def _():
            a_copy(1, col, chunk, True).start()
    for peer in peers:
        b_copy(peer, row).start()
    for chunk in range(CHUNKS):
        a_copy(2, col, chunk, True).start()

    out[...] = jnp.zeros_like(out)
    own_a.wait()
    own_b.wait()

    def multiply(block, chunk):
        part = pl.ds(pl.multiple_of(chunk * size, size), size)
        source = lax.div(block, per_b)
        offset = pl.multiple_of(lax.rem(block, per_b) * a_depth, a_depth)
        depth = pl.ds(offset, a_depth)
        high, low = split(a_all[block, part, :])
        right_high = b_high[source, depth, :]
        right_low = b_low[source, depth, :]
        dot = functools.partial(jnp.dot, preferred_element_type=jnp.float32)
        out[part, :] += (dot(low, right_high) + dot(high, right_low)) + dot(high, right_high)

    def split_b(source):
        @pl.loop(0, b_depth // 128)
        def _(index):
            part = pl.ds(pl.multiple_of(index * 128, 128), 128)
            high, low = split(b_all[source, part, :])
            b_high[source, part, :] = high
            b_low[source, part, :] = low

    def multiply_block(block):
        @pl.loop(0, CHUNKS)
        def _(chunk):
            multiply(block, chunk)

    for distance in range(1, chips - 1):
        for chunk in range(CHUNKS):
            @pl.when(left_valid(distance))
            def _():
                block = col - 2 * distance
                a_wait(block, chunk)

                @pl.when(right_valid(1))
                def _():
                    a_copy(0, block, chunk, False).start()
                a_copy(2, block, chunk, False).start()

            @pl.when(right_valid(distance))
            def _():
                block = col + 2 * distance
                a_wait(block, chunk)

                @pl.when(left_valid(1))
                def _():
                    a_copy(1, block, chunk, False).start()
                a_copy(2, block, chunk, False).start()

    split_b(row)
    for peer in peers:
        b_copy(peer, peer).wait_recv()
        split_b(peer)

    for chunk in range(CHUNKS):
        a_wait(partner, chunk)
    multiply_block(col)
    multiply_block(partner)
    for distance in range(1, chips - 1):
        for valid, step in ((left_valid, -2), (right_valid, 2)):
            @pl.when(valid(distance))
            def _():
                for chunk in range(CHUNKS):
                    a_wait(partner + step * distance, chunk)
                multiply_block(col + step * distance)
                multiply_block(partner + step * distance)

    if chips > 1:
        for valid, step in ((left_valid, -2), (right_valid, 2)):
            @pl.when(valid(chips - 1))
            def _():
                block = col + step * (chips - 1)
                other = partner + step * (chips - 1)
                for chunk in range(CHUNKS):
                    a_wait(block, chunk)
                    a_copy(2, block, chunk, False).start()
                    multiply(block, chunk)
                    a_wait(other, chunk)
                    multiply(other, chunk)

    for peer in peers:
        b_copy(peer, row).wait_send()
    for chunk in range(CHUNKS):
        a_copy(2, col, chunk, True).wait_send()
        for distance in range(0, chips):
            @pl.when(left_valid(distance) & right_valid(1))
            def _():
                a_copy(0, col - 2 * distance, chunk, False).wait_send()

            @pl.when(right_valid(distance) & left_valid(1))
            def _():
                a_copy(1, col + 2 * distance, chunk, False).wait_send()
        for distance in range(1, chips):
            @pl.when(left_valid(distance))
            def _():
                a_copy(2, col - 2 * distance, chunk, False).wait_send()

            @pl.when(right_valid(distance))
            def _():
                a_copy(2, col + 2 * distance, chunk, False).wait_send()


def body(rows, cols, left_matrix, right_matrix):
    height, a_depth = left_matrix.shape
    b_depth, width = right_matrix.shape
    return pl.pallas_call(
        functools.partial(kernel, rows, cols),
        out_shape=jax.ShapeDtypeStruct((height, width), jnp.float32),
        in_specs=[pl.BlockSpec(memory_space=pl.ANY)] * 2,
        out_specs=pl.BlockSpec(memory_space=pltpu.VMEM),
        scratch_shapes=[
            pltpu.VMEM((cols, height, a_depth), jnp.float32),
            pltpu.VMEM((rows, b_depth, width), jnp.float32),
            pltpu.VMEM((rows, b_depth, width), jnp.bfloat16),
            pltpu.VMEM((rows, b_depth, width), jnp.bfloat16),
            pltpu.SemaphoreType.DMA((cols, CHUNKS)),
            pltpu.SemaphoreType.DMA((3, cols, CHUNKS)),
            pltpu.SemaphoreType.DMA((rows,)),
            pltpu.SemaphoreType.DMA((rows,)),
            pltpu.SemaphoreType.DMA((2,)),
        ],
        compiler_params=pltpu.CompilerParams(
            collective_id=0, has_side_effects=True, vmem_limit_bytes=56 * 2**20),
    )(left_matrix, right_matrix)


STEPS = 16
FINE = 32
HEAD = 4
PRE = 1
GROUPS = 4
END_AT = 13
FAR_AT = 16
SUM_AT = 17
LANDED_AT = 20


def shared_kernel(a_in, b_in, out, a_all, b_all, b_high, b_low, c_all, c_high, c_low, partial,
                  a_recv, a_send, b_recv, b_send, c_recv, c_send, p_recv, p_send, local):
    row = lax.axis_index("row")
    col = lax.axis_index("col")
    core = lax.rem(col, 2)
    chip = lax.div(col, 2)
    partner = chip * 2 + 1 - core
    side = lax.div(chip, 2)
    y = lax.div(row, 2)
    x = lax.rem(row, 2)
    x_near = y * 2 + 1 - x
    y_near = (1 - y) * 2 + x
    far_corner = (1 - y) * 2 + 1 - x
    other_side = 1 - side
    end = 6 * side + core
    middle = 2 + 2 * side + core
    other_middle = 4 - 2 * side + core
    other_end = 6 - 6 * side + core
    swap = 1 - 2 * core
    is_end = (chip == 0) | (chip == 3)
    is_middle = (chip == 1) | (chip == 2)
    keeper = y == side
    donor = y == other_side
    height, a_depth = a_in.shape
    b_depth = b_in.shape[0]
    a_size = height // STEPS
    b_size = b_depth // FINE
    group = height // GROUPS

    def rows_of(index, size):
        return pl.ds(pl.multiple_of(index * size, size), size)

    def remote(source, target, send, recv, device):
        return pltpu.make_async_remote_copy(
            src_ref=source, dst_ref=target, send_sem=send, recv_sem=recv,
            device_id=device, device_id_type=MESH)

    def a_copy(kind, target, block, step, own=False):
        part = rows_of(step, a_size)
        return remote(a_in.at[part] if own else a_all.at[block, part], a_all.at[block, part],
                      a_send.at[kind, block], a_recv.at[block, step], {"col": target})

    def a_wait(block, step):
        a_copy(2, partner, block, step).wait_recv()

    def a_sent(kind, block):
        remote(a_all.at[block], a_all.at[block], a_send.at[kind, block], a_recv.at[block, 0],
               {"col": partner}).wait_send()

    def b_copy(kind, source, step, own=False):
        part = rows_of(step, b_size)
        return remote(b_in.at[part] if own else b_all.at[source, part], b_all.at[source, part],
                      b_send.at[kind, source], b_recv.at[source, step],
                      {"row": (x_near, y_near)[kind]})

    def b_wait(source, first, last):
        @pl.loop(first, last)
        def _(step):
            b_copy(0, source, step).wait_recv()

    def b_sent(kind, source, size):
        part = pl.ds(0, size)
        remote(b_all.at[source, part], b_all.at[source, part], b_send.at[kind, source],
               b_recv.at[source, 0], {"row": x_near}).wait_send()

    def c_copy(kind, slot, step, own=False):
        part = rows_of(step, b_size)
        target = ({"col": middle}, {"row": far_corner}, {"row": x_near}, {"row": y_near})[kind]
        return remote(b_in.at[part] if own else c_all.at[slot, part], c_all.at[slot, part],
                      c_send.at[kind], c_recv.at[slot, step], target)

    def c_sent(kind, size):
        part = pl.ds(0, size)
        remote(c_all.at[0, part], c_all.at[0, part], c_send.at[kind], c_recv.at[0, 0],
               {"row": x_near}).wait_send()

    def p_copy(step):
        part = rows_of(step, a_size)
        return remote(partial.at[part], partial.at[part], p_send, p_recv.at[step], {"col": end})

    def split_rows(source, part, full, high_all, low_all):
        high, low = split(full[source, part, :])
        high_all[source, part, :] = high
        low_all[source, part, :] = low

    def split_b(source, first, last):
        @pl.loop(first, last)
        def _(index):
            split_rows(source, rows_of(index, 128), b_all, b_high, b_low)

    dot = functools.partial(jnp.dot, preferred_element_type=jnp.float32)

    def term(part, block, high_all, low_all, source, half):
        depth = rows_of(half, a_depth)
        high, low = split(a_all[block, part, :])
        right_high = high_all[source, depth, :]
        right_low = low_all[source, depth, :]
        return (dot(low, right_high) + dot(high, right_low)) + dot(high, right_high)

    def job(source, half, index):
        part = rows_of(index, group)
        out[part, :] += term(part, 2 * source + half, b_high, b_low, source, half)

    barrier = pltpu.get_barrier_semaphore()

    def greet(target):
        pl.semaphore_signal(barrier, inc=1, device_id=target, device_id_type=MESH)

    greet({"col": partner})
    greet({"row": x_near})
    greet({"row": y_near})

    @pl.when(is_end)
    def _():
        greet({"col": middle})
        greet({"row": far_corner})

    @pl.when(is_middle)
    def _():
        greet({"col": end})
        greet({"col": other_middle})

    own_a = pltpu.make_async_copy(a_in, a_all.at[col], local.at[0])
    own_b = pltpu.make_async_copy(b_in, b_all.at[row], local.at[1])
    own_a.start()
    own_b.start()
    pl.semaphore_wait(barrier, 5)

    @pl.when(is_end)
    def _():
        first = 2 * side + x
        second = 2 * side + 1 - x

        for step in range(PRE):
            a_copy(0, middle, col, step, True).start()

        @pl.when(donor)
        def _():
            @pl.loop(0, FINE)
            def _(step):
                c_copy(1, x, step, True).start()
                c_copy(0, x, step, True).start()

            @pl.loop(PRE, STEPS)
            def _(step):
                a_copy(0, middle, col, step, True).start()

        @pl.when(keeper)
        def _():
            @pl.loop(0, FINE)
            def _(step):
                b_copy(0, row, step, True).start()
                b_copy(1, row, step, True).start()

        @pl.loop(0, STEPS)
        def _(step):
            a_copy(2, partner, col, step, True).start()
        out[...] = jnp.zeros_like(out)
        own_a.wait()
        own_b.wait()

        @pl.loop(0, LANDED_AT + STEPS)
        def _(t):
            @pl.when(keeper & (t < STEPS))
            def _():
                for index in range(2):
                    c_copy(0, 1 - x, 2 * t + index).wait_recv()
                    c_copy(0, 1 - x, 2 * t + index).start()

            @pl.when(keeper & (t == STEPS))
            def _():
                @pl.loop(PRE, STEPS)
                def _(step):
                    a_copy(0, middle, col, step, True).start()
                b_wait(x_near, 0, FINE)

            @pl.when(donor & (t < STEPS))
            def _():
                for index in range(2):
                    b_copy(0, y_near, 2 * t + index).wait_recv()
                    b_copy(0, y_near, 2 * t + index).start()

            @pl.when(t < STEPS)
            def _():
                a_wait(middle, t)
                a_copy(2, partner, middle, t).start()
                a_wait(end + swap, t)

            @pl.when((t >= 1) & (t < STEPS + 1))
            def _():
                a_wait(middle + swap, t - 1)

            @pl.when(t == STEPS + 1)
            def _():
                split_b(first, 0, 8)

            @pl.when((t >= STEPS + 2) & (t < STEPS + 10))
            def _():
                u = t - STEPS - 2
                job(first, lax.div(u, GROUPS), lax.rem(u, GROUPS))

            @pl.when(donor & (t == STEPS + 12))
            def _():
                b_wait(far_corner, 0, FINE // 2)

            @pl.when(t == STEPS + 12)
            def _():
                split_b(second, 0, 4)

            @pl.when((t >= STEPS + 13) & (t < STEPS + 17))
            def _():
                job(second, 0, t - STEPS - 13)

            @pl.when(donor & (t == STEPS + 18))
            def _():
                b_wait(far_corner, FINE // 2, FINE)

            @pl.when(t == STEPS + 18)
            def _():
                split_b(second, 4, 8)

                @pl.loop(0, GROUPS)
                def _(index):
                    job(second, 1, index)

            @pl.when(t >= LANDED_AT)
            def _():
                part = rows_of(t - LANDED_AT, a_size)
                p_copy(t - LANDED_AT).wait_recv()
                out[part, :] += partial[part, :]

        @pl.when(donor)
        def _():
            c_sent(0, b_depth)
            c_sent(1, b_depth)
            b_sent(0, y_near, b_depth)

        @pl.when(keeper)
        def _():
            c_sent(0, b_depth)
            b_sent(0, row, b_depth)
            b_sent(1, row, b_depth)
        a_sent(0, col)
        a_sent(2, col)
        a_sent(2, middle)

    @pl.when(is_middle)
    def _():
        inner = (row == 1) | (row == 2)
        slot = lax.rem(x + jnp.where(keeper, 1, 0), 2)

        @pl.loop(0, STEPS)
        def _(step):
            a_copy(0, other_middle, col, step, True).start()
            a_copy(1, end, col, step, True).start()

            @pl.when(step < HEAD)
            def _():
                b_copy(0, row, step, True).start()
                b_copy(1, row, step, True).start()
            a_copy(2, partner, col, step, True).start()
        out[...] = jnp.zeros_like(out)
        own_a.wait()
        own_b.wait()
        split_b(row, 0, 8)
        for step in range(PRE):
            a_wait(end, step)
            a_copy(0, other_middle, end, step).start()
            a_copy(2, partner, end, step).start()

        def sequence(s):
            late = s >= 28
            q = jnp.where(s >= 23, s - 14, s - 8)
            g, w = lax.div(q, 3), lax.rem(q, 3)
            last = (s >= 17) & (s < 23) | (s == 26) | (s == 27)
            v = jnp.where(s >= 26, s - 20, s - 17)
            near = lambda p: jnp.where(p == 0, x_near, y_near)
            u = lax.rem(s, 8)
            source = jnp.where(inner, row, near(lax.div(u, GROUPS)))
            half = jnp.where(inner, lax.div(u, GROUPS), 0)
            index = lax.rem(u, GROUPS)
            mid = (s >= 8) & (s < 28)
            pair = mid & (w < 2)
            source = jnp.where(mid, jnp.where(w < 2, jnp.where(inner, near(w), row), far_corner), source)
            half = jnp.where(mid, jnp.where(pair & ~inner, w, 0), half)
            index = jnp.where(mid, g, index)
            source = jnp.where(last, near(lax.rem(v, 2)), source)
            half = jnp.where(last, 1, half)
            index = jnp.where(last, lax.div(v, 2), index)
            source = jnp.where(late, far_corner, source)
            half = jnp.where(late, 1, half)
            index = jnp.where(late, s - 28, index)
            job(source, half, index)

        def until(t):
            total = 0
            for when, count in ((17, 2), (18, 2), (19, 2), (20, 2), (21, 2), (23, 1), (25, 2), (26, 1),
                                (29, 2), (30, 2), (31, 2), (32, 3)):
                total = total + jnp.where(t >= when, count, 0)
            return total

        @pl.loop(0, SUM_AT + STEPS)
        def _(t):
            @pl.when(t < STEPS)
            def _():
                for index in range(2):
                    c_copy(0, slot, 2 * t + index).wait_recv()
                    c_copy(2 + index, slot, 2 * t + index).start()

                @pl.when(t < FINE // 2 - HEAD)
                def _():
                    b_copy(0, row, HEAD + t, True).start()
                    b_copy(1, row, HEAD + t, True).start()
                a_wait(other_middle, t)
                a_copy(2, partner, other_middle, t).start()
                split_rows(slot, rows_of(t, 2 * b_size), c_all, c_high, c_low)

            @pl.when(t == STEPS)
            def _():
                b_wait(x_near, 0, FINE // 2)
                b_wait(y_near, 0, FINE // 2)

                @pl.loop(0, FINE // 4)
                def _(step):
                    b_copy(1, x_near, step).start()
                    b_copy(0, y_near, FINE // 4 + step).start()

                @pl.loop(0, FINE // 2)
                def _(step):
                    b_copy(0, row, FINE // 2 + step, True).start()
                    b_copy(1, row, FINE // 2 + lax.rem(step + FINE // 4, FINE // 2), True).start()
                split_b(x_near, 0, 4)
                split_b(y_near, 0, 4)

            @pl.when((t >= END_AT + PRE) & (t < END_AT + STEPS))
            def _():
                a_wait(end, t - END_AT)
                a_copy(0, other_middle, end, t - END_AT).start()
                a_copy(2, partner, end, t - END_AT).start()

            @pl.when((t >= FAR_AT) & (t < FAR_AT + STEPS))
            def _():
                a_wait(other_end, t - FAR_AT)
                a_copy(2, partner, other_end, t - FAR_AT).start()

            @pl.when((t >= 2) & (t < STEPS + 2))
            def _():
                a_wait(middle + swap, t - 2)
                a_wait(other_middle + swap, t - 2)
                for index in range(2):
                    c_copy(0, 1 - slot, 2 * (t - 2) + index).wait_recv()
                split_rows(1 - slot, rows_of(t - 2, 2 * b_size), c_all, c_high, c_low)

            @pl.when((t > END_AT) & (t < END_AT + 1 + STEPS))
            def _():
                a_wait(end + swap, t - END_AT - 1)

            @pl.when(t == 22)
            def _():
                b_wait(far_corner, 0, FINE // 2)
                split_b(far_corner, 0, 4)

            @pl.when(t == 26)
            def _():
                b_wait(x_near, FINE // 2, FINE // 4 * 3)
                b_wait(y_near, FINE // 4 * 3, FINE)

                @pl.loop(0, FINE // 4)
                def _(step):
                    b_copy(1, x_near, FINE // 2 + step).start()
                    b_copy(0, y_near, FINE // 4 * 3 + step).start()

            @pl.when(t == 29)
            def _():
                b_wait(x_near, FINE // 4 * 3, FINE)
                b_wait(y_near, FINE // 2, FINE // 4 * 3)
                split_b(x_near, 4, 8)
                split_b(y_near, 4, 8)

            @pl.when(t >= SUM_AT)
            def _():
                step = t - SUM_AT
                part = rows_of(step, a_size)
                a_wait(other_end + swap, step)
                value = None
                for index in range(4):
                    piece = term(part, 4 * other_side + index, c_high, c_low, index // 2, index % 2)
                    value = piece if value is None else value + piece
                partial[part, :] = value

                @pl.loop(until(t - 1), until(t))
                def _(s):
                    sequence(s)
                p_copy(step).start()

        b_wait(far_corner, FINE // 2, FINE)
        split_b(far_corner, 4, 8)

        @pl.loop(until(SUM_AT + STEPS), 8 * GROUPS)
        def _(s):
            sequence(s)

        for kind in range(3):
            a_sent(kind, col)
        a_sent(2, other_middle)
        a_sent(0, end)
        a_sent(2, end)
        a_sent(2, other_end)
        c_sent(2, b_depth // 2)
        c_sent(3, b_depth // 2)
        b_sent(0, row, b_depth)
        b_sent(1, row, b_depth)
        b_sent(0, y_near, b_depth // 2)
        b_sent(1, x_near, b_depth // 2)
        remote(partial, partial, p_send, p_recv.at[0], {"col": end}).wait_send()


def shared_body(left_matrix, right_matrix):
    height, a_depth = left_matrix.shape
    b_depth, width = right_matrix.shape
    dma = pltpu.SemaphoreType.DMA
    return pl.pallas_call(
        shared_kernel,
        out_shape=jax.ShapeDtypeStruct((height, width), jnp.float32),
        in_specs=[pl.BlockSpec(memory_space=pl.ANY)] * 2,
        out_specs=pl.BlockSpec(memory_space=pltpu.VMEM),
        scratch_shapes=[
            pltpu.VMEM((8, height, a_depth), jnp.float32),
            pltpu.VMEM((4, b_depth, width), jnp.float32),
            pltpu.VMEM((4, b_depth, width), jnp.bfloat16),
            pltpu.VMEM((4, b_depth, width), jnp.bfloat16),
            pltpu.VMEM((2, b_depth, width), jnp.float32),
            pltpu.VMEM((2, b_depth, width), jnp.bfloat16),
            pltpu.VMEM((2, b_depth, width), jnp.bfloat16),
            pltpu.VMEM((height, width), jnp.float32),
            dma((8, STEPS)), dma((3, 8)), dma((4, FINE)), dma((2, 4)),
            dma((2, FINE)), dma((4,)), dma((STEPS,)), dma(()), dma((2,)),
        ],
        compiler_params=pltpu.CompilerParams(
            collective_id=1, has_side_effects=True, vmem_limit_bytes=60 * 2**20),
    )(left_matrix, right_matrix)


def solution(mesh):
    placed = (P("row", "col"), P("row", "col"))
    rows, cols = mesh.shape["row"], mesh.shape["col"]
    part = shared_body if (rows, cols) == (4, 8) else functools.partial(body, rows, cols)
    return jax.shard_map(
        part, mesh=mesh, in_specs=placed, out_specs=P("row", "col"), check_vma=False
    )
```

```python
import functools

import jax
import jax.numpy as jnp
from jax import lax
from jax.experimental import pallas as pl
from jax.experimental.pallas import tpu as pltpu
from jax.sharding import PartitionSpec as P

MESH = pl.DeviceIdType.MESH
CHUNKS = 4


def split(value):
    high = value.astype(jnp.bfloat16)
    low = (value - high.astype(jnp.float32)).astype(jnp.bfloat16)
    return high, low


def kernel(rows, cols, a_in, b_in, out, a_all, b_all, b_high, b_low,
           a_recv, a_send, b_recv, b_send, local):
    row = lax.axis_index("row")
    col = lax.axis_index("col")
    core = lax.rem(col, 2)
    chip = lax.div(col, 2)
    chips = cols // 2
    height, a_depth = a_in.shape
    b_depth = b_in.shape[0]
    per_b = b_depth // a_depth
    size = height // CHUNKS
    partner = chip * 2 + 1 - core

    def left_valid(distance):
        return chip >= distance

    def right_valid(distance):
        return chip + distance < chips

    def a_copy(kind, block, chunk, own):
        part = pl.ds(chunk * size, size)
        target = (col + 2, col - 2, partner)[kind]
        return pltpu.make_async_remote_copy(
            src_ref=a_in.at[part] if own else a_all.at[block, part],
            dst_ref=a_all.at[block, part],
            send_sem=a_send.at[kind, block, chunk],
            recv_sem=a_recv.at[block, chunk],
            device_id={"col": target}, device_id_type=MESH)

    def a_wait(block, chunk):
        a_copy(2, block, chunk, False).wait_recv()

    def b_copy(peer, source):
        return pltpu.make_async_remote_copy(
            src_ref=b_in, dst_ref=b_all.at[source],
            send_sem=b_send.at[peer], recv_sem=b_recv.at[source],
            device_id={"row": peer}, device_id_type=MESH)

    barrier = pltpu.get_barrier_semaphore()

    @pl.when(chip > 0)
    def _():
        pl.semaphore_signal(barrier, inc=1, device_id={"col": col - 2}, device_id_type=MESH)

    @pl.when(chip < chips - 1)
    def _():
        pl.semaphore_signal(barrier, inc=1, device_id={"col": col + 2}, device_id_type=MESH)

    pl.semaphore_signal(barrier, inc=1, device_id={"col": partner}, device_id_type=MESH)
    peers = [lax.rem(row + offset, rows) for offset in range(1, rows)]
    for peer in peers:
        pl.semaphore_signal(barrier, inc=1, device_id={"row": peer}, device_id_type=MESH)
    own_a = pltpu.make_async_copy(a_in, a_all.at[col], local.at[0])
    own_b = pltpu.make_async_copy(b_in, b_all.at[row], local.at[1])
    own_a.start()
    own_b.start()
    near = jnp.where(chip > 0, 1, 0) + jnp.where(chip < chips - 1, 1, 0)
    pl.semaphore_wait(barrier, rows + near)

    for chunk in range(CHUNKS):
        @pl.when(right_valid(1))
        def _():
            a_copy(0, col, chunk, True).start()

        @pl.when(left_valid(1))
        def _():
            a_copy(1, col, chunk, True).start()
    for peer in peers:
        b_copy(peer, row).start()
    for chunk in range(CHUNKS):
        a_copy(2, col, chunk, True).start()

    out[...] = jnp.zeros_like(out)
    own_a.wait()
    own_b.wait()

    def multiply(block, chunk):
        part = pl.ds(pl.multiple_of(chunk * size, size), size)
        source = lax.div(block, per_b)
        offset = pl.multiple_of(lax.rem(block, per_b) * a_depth, a_depth)
        depth = pl.ds(offset, a_depth)
        high, low = split(a_all[block, part, :])
        right_high = b_high[source, depth, :]
        right_low = b_low[source, depth, :]
        dot = functools.partial(jnp.dot, preferred_element_type=jnp.float32)
        out[part, :] += (dot(low, right_high) + dot(high, right_low)) + dot(high, right_high)

    def split_b(source):
        @pl.loop(0, b_depth // 128)
        def _(index):
            part = pl.ds(pl.multiple_of(index * 128, 128), 128)
            high, low = split(b_all[source, part, :])
            b_high[source, part, :] = high
            b_low[source, part, :] = low

    def multiply_block(block):
        @pl.loop(0, CHUNKS)
        def _(chunk):
            multiply(block, chunk)

    for distance in range(1, chips - 1):
        for chunk in range(CHUNKS):
            @pl.when(left_valid(distance))
            def _():
                block = col - 2 * distance
                a_wait(block, chunk)

                @pl.when(right_valid(1))
                def _():
                    a_copy(0, block, chunk, False).start()
                a_copy(2, block, chunk, False).start()

            @pl.when(right_valid(distance))
            def _():
                block = col + 2 * distance
                a_wait(block, chunk)

                @pl.when(left_valid(1))
                def _():
                    a_copy(1, block, chunk, False).start()
                a_copy(2, block, chunk, False).start()

    split_b(row)
    for peer in peers:
        b_copy(peer, peer).wait_recv()
        split_b(peer)

    for chunk in range(CHUNKS):
        a_wait(partner, chunk)
    multiply_block(col)
    multiply_block(partner)
    for distance in range(1, chips - 1):
        for valid, step in ((left_valid, -2), (right_valid, 2)):
            @pl.when(valid(distance))
            def _():
                for chunk in range(CHUNKS):
                    a_wait(partner + step * distance, chunk)
                multiply_block(col + step * distance)
                multiply_block(partner + step * distance)

    if chips > 1:
        for valid, step in ((left_valid, -2), (right_valid, 2)):
            @pl.when(valid(chips - 1))
            def _():
                block = col + step * (chips - 1)
                other = partner + step * (chips - 1)
                for chunk in range(CHUNKS):
                    a_wait(block, chunk)
                    a_copy(2, block, chunk, False).start()
                    multiply(block, chunk)
                    a_wait(other, chunk)
                    multiply(other, chunk)

    for peer in peers:
        b_copy(peer, row).wait_send()
    for chunk in range(CHUNKS):
        a_copy(2, col, chunk, True).wait_send()
        for distance in range(0, chips):
            @pl.when(left_valid(distance) & right_valid(1))
            def _():
                a_copy(0, col - 2 * distance, chunk, False).wait_send()

            @pl.when(right_valid(distance) & left_valid(1))
            def _():
                a_copy(1, col + 2 * distance, chunk, False).wait_send()
        for distance in range(1, chips):
            @pl.when(left_valid(distance))
            def _():
                a_copy(2, col - 2 * distance, chunk, False).wait_send()

            @pl.when(right_valid(distance))
            def _():
                a_copy(2, col + 2 * distance, chunk, False).wait_send()


def body(rows, cols, left_matrix, right_matrix):
    height, a_depth = left_matrix.shape
    b_depth, width = right_matrix.shape
    return pl.pallas_call(
        functools.partial(kernel, rows, cols),
        out_shape=jax.ShapeDtypeStruct((height, width), jnp.float32),
        in_specs=[pl.BlockSpec(memory_space=pltpu.HBM)] * 2,
        out_specs=pl.BlockSpec(memory_space=pltpu.VMEM),
        scratch_shapes=[
            pltpu.VMEM((cols, height, a_depth), jnp.float32),
            pltpu.VMEM((rows, b_depth, width), jnp.float32),
            pltpu.VMEM((rows, b_depth, width), jnp.bfloat16),
            pltpu.VMEM((rows, b_depth, width), jnp.bfloat16),
            pltpu.SemaphoreType.DMA((cols, CHUNKS)),
            pltpu.SemaphoreType.DMA((3, cols, CHUNKS)),
            pltpu.SemaphoreType.DMA((rows,)),
            pltpu.SemaphoreType.DMA((rows,)),
            pltpu.SemaphoreType.DMA((2,)),
        ],
        compiler_params=pltpu.CompilerParams(
            collective_id=0, has_side_effects=True, vmem_limit_bytes=56 * 2**20),
    )(left_matrix, right_matrix)


STEPS = 16
FINE = 32
HEAD = 8
PRE = 1
MORE = 1
GROUPS = 4
LACK = 2
LENT = FINE // 2 - LACK
LENT_AT = 3
LACK_AT = 5
RELAY_AT = 14
LAST_AT = 26
END_AT = 14
FAR_AT = 16
SUM_AT = 17
LANDED_AT = 20


def shared_kernel(a_in, b_in, out, a_all, b_all, b_high, b_low, c_all, c_high, c_low, partial,
                  a_recv, a_send, b_recv, b_send, c_recv, c_send, p_recv, p_send, local):
    row = lax.axis_index("row")
    col = lax.axis_index("col")
    core = lax.rem(col, 2)
    chip = lax.div(col, 2)
    partner = chip * 2 + 1 - core
    side = lax.div(chip, 2)
    y = lax.div(row, 2)
    x = lax.rem(row, 2)
    x_near = y * 2 + 1 - x
    y_near = (1 - y) * 2 + x
    far_corner = (1 - y) * 2 + 1 - x
    other_side = 1 - side
    end = 6 * side + core
    middle = 2 + 2 * side + core
    other_middle = 4 - 2 * side + core
    other_end = 6 - 6 * side + core
    swap = 1 - 2 * core
    is_end = (chip == 0) | (chip == 3)
    is_middle = (chip == 1) | (chip == 2)
    keeper = y == side
    donor = y == other_side
    height, a_depth = a_in.shape
    b_depth = b_in.shape[0]
    a_size = height // STEPS
    b_size = b_depth // FINE
    group = height // GROUPS

    def rows_of(index, size):
        return pl.ds(pl.multiple_of(index * size, size), size)

    def remote(source, target, send, recv, device):
        return pltpu.make_async_remote_copy(
            src_ref=source, dst_ref=target, send_sem=send, recv_sem=recv,
            device_id=device, device_id_type=MESH)

    def a_copy(kind, target, block, step, own=False):
        part = rows_of(step, a_size)
        return remote(a_in.at[part] if own else a_all.at[block, part], a_all.at[block, part],
                      a_send.at[kind, block], a_recv.at[block, step], {"col": target})

    def a_wait(block, step):
        a_copy(2, partner, block, step).wait_recv()

    def a_sent(kind, block):
        remote(a_all.at[block], a_all.at[block], a_send.at[kind, block], a_recv.at[block, 0],
               {"col": partner}).wait_send()

    def b_copy(kind, source, step, own=False):
        part = rows_of(step, b_size)
        return remote(b_in.at[part] if own else b_all.at[source, part], b_all.at[source, part],
                      b_send.at[kind, source], b_recv.at[source, step],
                      {"row": (x_near, y_near)[kind]})

    def b_wait(source, first, last):
        @pl.loop(first, last)
        def _(step):
            b_copy(0, source, step).wait_recv()

    def b_sent(kind, source, size):
        part = pl.ds(0, size)
        remote(b_all.at[source, part], b_all.at[source, part], b_send.at[kind, source],
               b_recv.at[source, 0], {"row": x_near}).wait_send()

    def c_copy(kind, slot, step, own=False):
        part = rows_of(step, b_size)
        target = ({"col": middle}, {"row": far_corner}, {"row": x_near}, {"row": y_near})[kind]
        return remote(b_in.at[part] if own else c_all.at[slot, part], c_all.at[slot, part],
                      c_send.at[kind], c_recv.at[slot, step], target)

    def c_sent(kind, size):
        part = pl.ds(0, size)
        remote(c_all.at[0, part], c_all.at[0, part], c_send.at[kind], c_recv.at[0, 0],
               {"row": x_near}).wait_send()

    def lent(step, held):
        return step + jnp.where(held & (step < 2 * LACK), 0, 2 * LACK)

    def p_copy(step):
        part = rows_of(step, a_size)
        return remote(partial.at[part], partial.at[part], p_send, p_recv.at[step], {"col": end})

    def split_rows(source, part, full, high_all, low_all):
        high, low = split(full[source, part, :])
        high_all[source, part, :] = high
        low_all[source, part, :] = low

    def split_b(source, first, last):
        @pl.loop(first, last)
        def _(index):
            split_rows(source, rows_of(index, 128), b_all, b_high, b_low)

    dot = functools.partial(jnp.dot, preferred_element_type=jnp.float32)

    def term(part, block, high_all, low_all, source, half):
        depth = rows_of(half, a_depth)
        high, low = split(a_all[block, part, :])
        right_high = high_all[source, depth, :]
        right_low = low_all[source, depth, :]
        return (dot(low, right_high) + dot(high, right_low)) + dot(high, right_high)

    def job(source, half, index):
        part = rows_of(index, group)
        out[part, :] += term(part, 2 * source + half, b_high, b_low, source, half)

    barrier = pltpu.get_barrier_semaphore()

    def greet(target):
        pl.semaphore_signal(barrier, inc=1, device_id=target, device_id_type=MESH)

    greet({"col": partner})
    greet({"row": x_near})
    greet({"row": y_near})

    @pl.when(is_end)
    def _():
        greet({"col": middle})
        greet({"row": far_corner})

    @pl.when(is_middle)
    def _():
        greet({"col": end})
        greet({"col": other_middle})

    own_a = pltpu.make_async_copy(a_in, a_all.at[col], local.at[0])
    own_b = pltpu.make_async_copy(b_in, b_all.at[row], local.at[1])
    own_a.start()
    own_b.start()
    pl.semaphore_wait(barrier, 5)

    @pl.when(is_end)
    def _():
        first = 2 * side + x
        second = 2 * side + 1 - x

        for step in range(PRE):
            a_copy(0, middle, col, step, True).start()

        @pl.when(donor)
        def _():
            @pl.loop(0, 2 * LENT)
            def _(step):
                c_copy(1, x, lent(step, True), True).start()
                c_copy(0, x, lent(step, False), True).start()

            @pl.loop(PRE, STEPS)
            def _(step):
                a_copy(0, middle, col, step, True).start()

        @pl.when(keeper)
        def _():
            @pl.loop(0, FINE)
            def _(step):
                b_copy(0, row, step, True).start()
                b_copy(1, row, step, True).start()

            for step in range(PRE, PRE + MORE):
                a_copy(0, middle, col, step, True).start()

        @pl.loop(0, STEPS)
        def _(step):
            a_copy(2, partner, col, step, True).start()
        out[...] = jnp.zeros_like(out)
        own_a.wait()
        own_b.wait()

        @pl.loop(0, LANDED_AT + STEPS)
        def _(t):
            @pl.when(keeper & (t < LENT))
            def _():
                for index in range(2):
                    chunk = lent(2 * t + index, True)
                    c_copy(0, 1 - x, chunk).wait_recv()
                    c_copy(0, 1 - x, chunk).start()

            @pl.when(keeper & (t == LENT))
            def _():
                @pl.loop(PRE + MORE, STEPS)
                def _(step):
                    a_copy(0, middle, col, step, True).start()

            @pl.when(keeper & (t == STEPS + 1))
            def _():
                b_wait(x_near, 0, FINE)

            @pl.when(donor & (t < STEPS))
            def _():
                for index in range(2):
                    b_copy(0, y_near, 2 * t + index).wait_recv()
                    b_copy(0, y_near, 2 * t + index).start()

            @pl.when(t < STEPS)
            def _():
                a_wait(middle, t)
                a_copy(2, partner, middle, t).start()
                a_wait(end + swap, t)

            @pl.when((t >= 1) & (t < STEPS + 1))
            def _():
                a_wait(middle + swap, t - 1)

            @pl.when(t == STEPS + 1)
            def _():
                split_b(first, 0, 8)

            @pl.when((t >= STEPS + 2) & (t < STEPS + 10))
            def _():
                u = t - STEPS - 2
                job(first, lax.div(u, GROUPS), lax.rem(u, GROUPS))

            @pl.when(donor & (t == STEPS + 12))
            def _():
                b_wait(far_corner, 0, FINE // 2)

            @pl.when(t == STEPS + 12)
            def _():
                split_b(second, 0, 4)

            @pl.when((t >= STEPS + 13) & (t < STEPS + 17))
            def _():
                job(second, 0, t - STEPS - 13)

            @pl.when(donor & (t == STEPS + 18))
            def _():
                b_wait(far_corner, FINE // 2, FINE)

            @pl.when(t == STEPS + 18)
            def _():
                split_b(second, 4, 8)

                @pl.loop(0, GROUPS)
                def _(index):
                    job(second, 1, index)

            @pl.when(t >= LANDED_AT)
            def _():
                part = rows_of(t - LANDED_AT, a_size)
                p_copy(t - LANDED_AT).wait_recv()
                out[part, :] += partial[part, :]

        @pl.when(donor)
        def _():
            c_sent(0, 2 * LENT * b_size)
            c_sent(1, 2 * LENT * b_size)
            b_sent(0, y_near, b_depth)

        @pl.when(keeper)
        def _():
            c_sent(0, 2 * LENT * b_size)
            b_sent(0, row, b_depth)
            b_sent(1, row, b_depth)
        a_sent(0, col)
        a_sent(2, col)
        a_sent(2, middle)

    @pl.when(is_middle)
    def _():
        inner = (row == 1) | (row == 2)
        slot = lax.rem(x + jnp.where(keeper, 1, 0), 2)
        mine = jnp.where(keeper, 2 * LACK, 0)
        theirs = 2 * LACK - mine

        def within(chunk, start):
            return (chunk >= start) & (chunk < start + 2 * LACK)

        def c_split(which, step):
            split_rows(which, rows_of(step, 2 * b_size), c_all, c_high, c_low)

        def c_landed(chunk):
            c_copy(0, 1 - slot, chunk).wait_recv()

            @pl.when(within(chunk, mine) & (lax.rem(chunk, 2) == 0))
            def _():
                c_copy(2, 1 - slot, chunk).start()

            @pl.when(within(chunk, theirs) & (lax.rem(chunk, 2) == 1))
            def _():
                c_copy(3, 1 - slot, chunk).start()

        @pl.loop(0, STEPS)
        def _(step):
            a_copy(0, other_middle, col, step, True).start()
            a_copy(1, end, col, step, True).start()

            @pl.when(step < HEAD)
            def _():
                b_copy(0, row, step, True).start()
                b_copy(1, row, step, True).start()
            a_copy(2, partner, col, step, True).start()
        out[...] = jnp.zeros_like(out)
        own_a.wait()
        own_b.wait()
        split_b(row, 0, 8)
        for step in range(PRE):
            a_wait(end, step)
            a_copy(0, other_middle, end, step).start()
            a_copy(2, partner, end, step).start()

        def sequence(s):
            late = s >= 28
            q = jnp.where(s >= 23, s - 14, s - 8)
            g, w = lax.div(q, 3), lax.rem(q, 3)
            last = (s >= 17) & (s < 23) | (s == 26) | (s == 27)
            v = jnp.where(s >= 26, s - 20, s - 17)
            near = lambda p: jnp.where(p == 0, x_near, y_near)
            u = lax.rem(s, 8)
            source = jnp.where(inner, row, near(lax.div(u, GROUPS)))
            half = jnp.where(inner, lax.div(u, GROUPS), 0)
            index = lax.rem(u, GROUPS)
            mid = (s >= 8) & (s < 28)
            pair = mid & (w < 2)
            source = jnp.where(mid, jnp.where(w < 2, jnp.where(inner, near(w), row), far_corner), source)
            half = jnp.where(mid, jnp.where(pair & ~inner, w, 0), half)
            index = jnp.where(mid, g, index)
            source = jnp.where(last, near(lax.rem(v, 2)), source)
            half = jnp.where(last, 1, half)
            index = jnp.where(last, lax.div(v, 2), index)
            source = jnp.where(late, far_corner, source)
            half = jnp.where(late, 1, half)
            index = jnp.where(late, s - 28, index)
            job(source, half, index)

        def until(t):
            total = 0
            for when, count in ((17, 2), (18, 2), (19, 2), (20, 2), (21, 2), (23, 1), (24, 2), (25, 1),
                                (28, 2), (29, 2), (30, 2), (31, 2), (32, 1)):
                total = total + jnp.where(t >= when, count, 0)
            return total

        @pl.loop(0, SUM_AT + STEPS)
        def _(t):
            @pl.when(t < LENT)
            def _():
                for index in range(2):
                    chunk = lent(2 * t + index, keeper)
                    c_copy(0, slot, chunk).wait_recv()
                    both = within(chunk, theirs)

                    @pl.when(both | (lax.rem(chunk, 2) == 0))
                    def _():
                        c_copy(2, slot, chunk).start()

                    @pl.when(both | (lax.rem(chunk, 2) == 1))
                    def _():
                        c_copy(3, slot, chunk).start()
                c_split(slot, lax.div(lent(2 * t, keeper), 2))

            @pl.when(t < (FINE // 2 - HEAD) // 2)
            def _():
                for index in range(2):
                    b_copy(0, row, HEAD + 2 * t + index, True).start()
                    b_copy(1, row, HEAD + 2 * t + index, True).start()

            @pl.when(t < STEPS)
            def _():
                a_wait(other_middle, t)
                a_copy(2, partner, other_middle, t).start()

            @pl.when(t == RELAY_AT)
            def _():
                b_wait(x_near, 0, FINE // 4)
                b_wait(y_near, FINE // 4, FINE // 2)

                @pl.loop(0, FINE // 4)
                def _(step):
                    b_copy(1, x_near, step).start()
                    b_copy(0, y_near, FINE // 4 + step).start()

                @pl.loop(0, FINE // 2)
                def _(step):
                    b_copy(0, row, FINE // 2 + step, True).start()
                    b_copy(1, row, FINE // 2 + lax.rem(step + FINE // 4, FINE // 2), True).start()

            @pl.when(t == RELAY_AT + 2)
            def _():
                b_wait(x_near, FINE // 4, FINE // 2)
                b_wait(y_near, 0, FINE // 4)
                split_b(x_near, 0, 4)
                split_b(y_near, 0, 4)

            @pl.when((t >= END_AT + PRE) & (t < END_AT + STEPS))
            def _():
                a_wait(end, t - END_AT)
                a_copy(0, other_middle, end, t - END_AT).start()
                a_copy(2, partner, end, t - END_AT).start()

            @pl.when((t >= FAR_AT) & (t < FAR_AT + STEPS))
            def _():
                a_wait(other_end, t - FAR_AT)
                a_copy(2, partner, other_end, t - FAR_AT).start()

            @pl.when((t >= 2) & (t < STEPS + 2))
            def _():
                a_wait(middle + swap, t - 2)
                a_wait(other_middle + swap, t - 2)

            @pl.when((t >= LENT_AT) & (t < LENT_AT + LENT))
            def _():
                u = t - LENT_AT

                @pl.when(u < LACK)
                def _():
                    c_landed(2 * u)
                    c_landed(2 * u + 1)
                    c_split(1 - slot, u)
                c_landed(2 * LACK + 2 * u)
                c_landed(2 * LACK + 2 * u + 1)
                c_split(1 - slot, LACK + u)

            @pl.when((t >= LACK_AT) & (t < LACK_AT + LACK))
            def _():
                chunk = mine + 2 * (t - LACK_AT)
                c_copy(0, slot, chunk).wait_recv()
                c_copy(0, slot, chunk + 1).wait_recv()
                c_split(slot, lax.div(chunk, 2))

            @pl.when((t > END_AT) & (t < END_AT + 1 + STEPS))
            def _():
                a_wait(end + swap, t - END_AT - 1)

            @pl.when(t == 21)
            def _():
                b_wait(far_corner, 0, FINE // 2)
                split_b(far_corner, 0, 4)

            @pl.when(t == LAST_AT)
            def _():
                b_wait(x_near, FINE // 2, FINE // 4 * 3)
                b_wait(y_near, FINE // 4 * 3, FINE)

                @pl.loop(0, FINE // 4)
                def _(step):
                    b_copy(1, x_near, FINE // 2 + step).start()
                    b_copy(0, y_near, FINE // 4 * 3 + step).start()

            @pl.when(t == LAST_AT + 3)
            def _():
                b_wait(x_near, FINE // 4 * 3, FINE)
                b_wait(y_near, FINE // 2, FINE // 4 * 3)
                split_b(x_near, 4, 8)
                split_b(y_near, 4, 8)

            @pl.when(t >= SUM_AT)
            def _():
                step = t - SUM_AT
                a_wait(other_end + swap, step)

                @pl.when(lax.rem(step, 2) == 1)
                def _():
                    part = rows_of(lax.div(step, 2), 2 * a_size)
                    value = None
                    for index in range(4):
                        piece = term(part, 4 * other_side + index, c_high, c_low, index // 2, index % 2)
                        value = piece if value is None else value + piece
                    partial[part, :] = value
                    p_copy(step - 1).start()
                    p_copy(step).start()

                @pl.loop(until(t - 1), until(t))
                def _(s):
                    sequence(s)

        b_wait(far_corner, FINE // 2, FINE)
        split_b(far_corner, 4, 8)

        @pl.loop(until(SUM_AT + STEPS), 8 * GROUPS)
        def _(s):
            sequence(s)

        for kind in range(3):
            a_sent(kind, col)
        a_sent(2, other_middle)
        a_sent(0, end)
        a_sent(2, end)
        a_sent(2, other_end)
        c_sent(2, (FINE // 2 + LACK) * b_size)
        c_sent(3, (FINE // 2 + LACK) * b_size)
        b_sent(0, row, b_depth)
        b_sent(1, row, b_depth)
        b_sent(0, y_near, b_depth // 2)
        b_sent(1, x_near, b_depth // 2)
        remote(partial, partial, p_send, p_recv.at[0], {"col": end}).wait_send()


def shared_body(left_matrix, right_matrix):
    height, a_depth = left_matrix.shape
    b_depth, width = right_matrix.shape
    dma = pltpu.SemaphoreType.DMA
    return pl.pallas_call(
        shared_kernel,
        out_shape=jax.ShapeDtypeStruct((height, width), jnp.float32),
        in_specs=[pl.BlockSpec(memory_space=pltpu.HBM)] * 2,
        out_specs=pl.BlockSpec(memory_space=pltpu.VMEM),
        scratch_shapes=[
            pltpu.VMEM((8, height, a_depth), jnp.float32),
            pltpu.VMEM((4, b_depth, width), jnp.float32),
            pltpu.VMEM((4, b_depth, width), jnp.bfloat16),
            pltpu.VMEM((4, b_depth, width), jnp.bfloat16),
            pltpu.VMEM((2, b_depth, width), jnp.float32),
            pltpu.VMEM((2, b_depth, width), jnp.bfloat16),
            pltpu.VMEM((2, b_depth, width), jnp.bfloat16),
            pltpu.VMEM((height, width), jnp.float32),
            dma((8, STEPS)), dma((3, 8)), dma((4, FINE)), dma((2, 4)),
            dma((2, FINE)), dma((4,)), dma((STEPS,)), dma(()), dma((2,)),
        ],
        compiler_params=pltpu.CompilerParams(
            collective_id=1, has_side_effects=True, vmem_limit_bytes=48 * 2**20),
    )(left_matrix, right_matrix)


def solution(mesh):
    placed = (P("row", "col"), P("row", "col"))
    rows, cols = mesh.shape["row"], mesh.shape["col"]
    part = shared_body if (rows, cols) == (4, 8) else functools.partial(body, rows, cols)
    return jax.shard_map(
        part, mesh=mesh, in_specs=placed, out_specs=P("row", "col"), check_vma=False
    )
```

```python
import functools

import jax
import jax.numpy as jnp
from jax import lax
from jax.experimental import pallas as pl
from jax.experimental.pallas import tpu as pltpu
from jax.sharding import PartitionSpec as P

MESH = pl.DeviceIdType.MESH
CHUNKS = 4


def split(value):
    high = value.astype(jnp.bfloat16)
    low = (value - high.astype(jnp.float32)).astype(jnp.bfloat16)
    return high, low


def kernel(rows, cols, a_in, b_in, out, a_all, b_all, b_high, b_low,
           a_recv, a_send, b_recv, b_send, local):
    row = lax.axis_index("row")
    col = lax.axis_index("col")
    core = lax.rem(col, 2)
    chip = lax.div(col, 2)
    chips = cols // 2
    height, a_depth = a_in.shape
    b_depth = b_in.shape[0]
    per_b = b_depth // a_depth
    size = height // CHUNKS
    partner = chip * 2 + 1 - core

    def left_valid(distance):
        return chip >= distance

    def right_valid(distance):
        return chip + distance < chips

    def a_copy(kind, block, chunk, own):
        part = pl.ds(chunk * size, size)
        target = (col + 2, col - 2, partner)[kind]
        return pltpu.make_async_remote_copy(
            src_ref=a_in.at[part] if own else a_all.at[block, part],
            dst_ref=a_all.at[block, part],
            send_sem=a_send.at[kind, block, chunk],
            recv_sem=a_recv.at[block, chunk],
            device_id={"col": target}, device_id_type=MESH)

    def a_wait(block, chunk):
        a_copy(2, block, chunk, False).wait_recv()

    def b_copy(peer, source):
        return pltpu.make_async_remote_copy(
            src_ref=b_in, dst_ref=b_all.at[source],
            send_sem=b_send.at[peer], recv_sem=b_recv.at[source],
            device_id={"row": peer}, device_id_type=MESH)

    barrier = pltpu.get_barrier_semaphore()

    @pl.when(chip > 0)
    def _():
        pl.semaphore_signal(barrier, inc=1, device_id={"col": col - 2}, device_id_type=MESH)

    @pl.when(chip < chips - 1)
    def _():
        pl.semaphore_signal(barrier, inc=1, device_id={"col": col + 2}, device_id_type=MESH)

    pl.semaphore_signal(barrier, inc=1, device_id={"col": partner}, device_id_type=MESH)
    peers = [lax.rem(row + offset, rows) for offset in range(1, rows)]
    for peer in peers:
        pl.semaphore_signal(barrier, inc=1, device_id={"row": peer}, device_id_type=MESH)
    own_a = pltpu.make_async_copy(a_in, a_all.at[col], local.at[0])
    own_b = pltpu.make_async_copy(b_in, b_all.at[row], local.at[1])
    own_a.start()
    own_b.start()
    near = jnp.where(chip > 0, 1, 0) + jnp.where(chip < chips - 1, 1, 0)
    pl.semaphore_wait(barrier, rows + near)

    for chunk in range(CHUNKS):
        @pl.when(right_valid(1))
        def _():
            a_copy(0, col, chunk, True).start()

        @pl.when(left_valid(1))
        def _():
            a_copy(1, col, chunk, True).start()
    for peer in peers:
        b_copy(peer, row).start()
    for chunk in range(CHUNKS):
        a_copy(2, col, chunk, True).start()

    out[...] = jnp.zeros_like(out)
    own_a.wait()
    own_b.wait()

    def multiply(block, chunk):
        part = pl.ds(pl.multiple_of(chunk * size, size), size)
        source = lax.div(block, per_b)
        offset = pl.multiple_of(lax.rem(block, per_b) * a_depth, a_depth)
        depth = pl.ds(offset, a_depth)
        high, low = split(a_all[block, part, :])
        right_high = b_high[source, depth, :]
        right_low = b_low[source, depth, :]
        dot = functools.partial(jnp.dot, preferred_element_type=jnp.float32)
        out[part, :] += (dot(low, right_high) + dot(high, right_low)) + dot(high, right_high)

    def split_b(source):
        @pl.loop(0, b_depth // 128)
        def _(index):
            part = pl.ds(pl.multiple_of(index * 128, 128), 128)
            high, low = split(b_all[source, part, :])
            b_high[source, part, :] = high
            b_low[source, part, :] = low

    def multiply_block(block):
        @pl.loop(0, CHUNKS)
        def _(chunk):
            multiply(block, chunk)

    for distance in range(1, chips - 1):
        for chunk in range(CHUNKS):
            @pl.when(left_valid(distance))
            def _():
                block = col - 2 * distance
                a_wait(block, chunk)

                @pl.when(right_valid(1))
                def _():
                    a_copy(0, block, chunk, False).start()
                a_copy(2, block, chunk, False).start()

            @pl.when(right_valid(distance))
            def _():
                block = col + 2 * distance
                a_wait(block, chunk)

                @pl.when(left_valid(1))
                def _():
                    a_copy(1, block, chunk, False).start()
                a_copy(2, block, chunk, False).start()

    split_b(row)
    for peer in peers:
        b_copy(peer, peer).wait_recv()
        split_b(peer)

    for chunk in range(CHUNKS):
        a_wait(partner, chunk)
    multiply_block(col)
    multiply_block(partner)
    for distance in range(1, chips - 1):
        for valid, step in ((left_valid, -2), (right_valid, 2)):
            @pl.when(valid(distance))
            def _():
                for chunk in range(CHUNKS):
                    a_wait(partner + step * distance, chunk)
                multiply_block(col + step * distance)
                multiply_block(partner + step * distance)

    if chips > 1:
        for valid, step in ((left_valid, -2), (right_valid, 2)):
            @pl.when(valid(chips - 1))
            def _():
                block = col + step * (chips - 1)
                other = partner + step * (chips - 1)
                for chunk in range(CHUNKS):
                    a_wait(block, chunk)
                    a_copy(2, block, chunk, False).start()
                    multiply(block, chunk)
                    a_wait(other, chunk)
                    multiply(other, chunk)

    for peer in peers:
        b_copy(peer, row).wait_send()
    for chunk in range(CHUNKS):
        a_copy(2, col, chunk, True).wait_send()
        for distance in range(0, chips):
            @pl.when(left_valid(distance) & right_valid(1))
            def _():
                a_copy(0, col - 2 * distance, chunk, False).wait_send()

            @pl.when(right_valid(distance) & left_valid(1))
            def _():
                a_copy(1, col + 2 * distance, chunk, False).wait_send()
        for distance in range(1, chips):
            @pl.when(left_valid(distance))
            def _():
                a_copy(2, col - 2 * distance, chunk, False).wait_send()

            @pl.when(right_valid(distance))
            def _():
                a_copy(2, col + 2 * distance, chunk, False).wait_send()


def body(rows, cols, left_matrix, right_matrix):
    height, a_depth = left_matrix.shape
    b_depth, width = right_matrix.shape
    return pl.pallas_call(
        functools.partial(kernel, rows, cols),
        out_shape=jax.ShapeDtypeStruct((height, width), jnp.float32),
        in_specs=[pl.BlockSpec(memory_space=pltpu.HBM)] * 2,
        out_specs=pl.BlockSpec(memory_space=pltpu.VMEM),
        scratch_shapes=[
            pltpu.VMEM((cols, height, a_depth), jnp.float32),
            pltpu.VMEM((rows, b_depth, width), jnp.float32),
            pltpu.VMEM((rows, b_depth, width), jnp.bfloat16),
            pltpu.VMEM((rows, b_depth, width), jnp.bfloat16),
            pltpu.SemaphoreType.DMA((cols, CHUNKS)),
            pltpu.SemaphoreType.DMA((3, cols, CHUNKS)),
            pltpu.SemaphoreType.DMA((rows,)),
            pltpu.SemaphoreType.DMA((rows,)),
            pltpu.SemaphoreType.DMA((2,)),
        ],
        compiler_params=pltpu.CompilerParams(
            collective_id=0, has_side_effects=True, vmem_limit_bytes=56 * 2**20),
    )(left_matrix, right_matrix)


STEPS = 16
FINE = 32
HEAD = 8
PRE = 1
MORE = 1
GROUPS = 4
LACK = 2
LENT = FINE // 2 - LACK
LENT_AT = 3
LACK_AT = 5
OWN_AT = 14
NEAR_AT = 16
RELAY_AT = 21
LAST_AT = 24
FAR_B_AT = 28
END_AT = 14
FAR_AT = 16
SUM_AT = 16
LANDED_AT = 20


def shared_kernel(a_in, b_in, out, a_all, b_all, b_high, b_low, c_all, c_high, c_low, partial,
                  a_recv, a_send, b_recv, b_send, c_recv, c_send, p_recv, p_send, local):
    row = lax.axis_index("row")
    col = lax.axis_index("col")
    core = lax.rem(col, 2)
    chip = lax.div(col, 2)
    partner = chip * 2 + 1 - core
    side = lax.div(chip, 2)
    y = lax.div(row, 2)
    x = lax.rem(row, 2)
    x_near = y * 2 + 1 - x
    y_near = (1 - y) * 2 + x
    far_corner = (1 - y) * 2 + 1 - x
    other_side = 1 - side
    end = 6 * side + core
    middle = 2 + 2 * side + core
    other_middle = 4 - 2 * side + core
    other_end = 6 - 6 * side + core
    swap = 1 - 2 * core
    is_end = (chip == 0) | (chip == 3)
    is_middle = (chip == 1) | (chip == 2)
    keeper = y == side
    donor = y == other_side
    height, a_depth = a_in.shape
    b_depth = b_in.shape[0]
    a_size = height // STEPS
    b_size = b_depth // FINE
    group = height // GROUPS

    def rows_of(index, size):
        return pl.ds(pl.multiple_of(index * size, size), size)

    def remote(source, target, send, recv, device):
        return pltpu.make_async_remote_copy(
            src_ref=source, dst_ref=target, send_sem=send, recv_sem=recv,
            device_id=device, device_id_type=MESH)

    def a_copy(kind, target, block, step, own=False):
        part = rows_of(step, a_size)
        return remote(a_in.at[part] if own else a_all.at[block, part], a_all.at[block, part],
                      a_send.at[kind, block], a_recv.at[block, step], {"col": target})

    def a_wait(block, step):
        a_copy(2, partner, block, step).wait_recv()

    def a_sent(kind, block):
        remote(a_all.at[block], a_all.at[block], a_send.at[kind, block], a_recv.at[block, 0],
               {"col": partner}).wait_send()

    def b_copy(kind, source, step, own=False):
        part = rows_of(step, b_size)
        return remote(b_in.at[part] if own else b_all.at[source, part], b_all.at[source, part],
                      b_send.at[kind, source], b_recv.at[source, step],
                      {"row": (x_near, y_near)[kind]})

    def b_wait(source, first, last):
        @pl.loop(first, last)
        def _(step):
            b_copy(0, source, step).wait_recv()

    def b_sent(kind, source, size):
        part = pl.ds(0, size)
        remote(b_all.at[source, part], b_all.at[source, part], b_send.at[kind, source],
               b_recv.at[source, 0], {"row": x_near}).wait_send()

    def c_copy(kind, slot, step, own=False):
        part = rows_of(step, b_size)
        target = ({"col": middle}, {"row": far_corner}, {"row": x_near}, {"row": y_near})[kind]
        return remote(b_in.at[part] if own else c_all.at[slot, part], c_all.at[slot, part],
                      c_send.at[kind], c_recv.at[slot, step], target)

    def c_sent(kind, size):
        part = pl.ds(0, size)
        remote(c_all.at[0, part], c_all.at[0, part], c_send.at[kind], c_recv.at[0, 0],
               {"row": x_near}).wait_send()

    def lent(step, held):
        return step + jnp.where(held & (step < 2 * LACK), 0, 2 * LACK)

    def p_copy(step):
        part = rows_of(step, a_size)
        return remote(partial.at[part], partial.at[part], p_send, p_recv.at[step], {"col": end})

    def split_rows(source, part, full, high_all, low_all):
        high, low = split(full[source, part, :])
        high_all[source, part, :] = high
        low_all[source, part, :] = low

    def split_b(source, first, last):
        @pl.loop(first, last)
        def _(index):
            split_rows(source, rows_of(index, 128), b_all, b_high, b_low)

    dot = functools.partial(jnp.dot, preferred_element_type=jnp.float32)

    def term(part, block, high_all, low_all, source, half):
        depth = rows_of(half, a_depth)
        high, low = split(a_all[block, part, :])
        right_high = high_all[source, depth, :]
        right_low = low_all[source, depth, :]
        return (dot(low, right_high) + dot(high, right_low)) + dot(high, right_high)

    def job(source, half, index, size=group):
        part = rows_of(index, size)
        out[part, :] += term(part, 2 * source + half, b_high, b_low, source, half)

    barrier = pltpu.get_barrier_semaphore()

    def greet(target):
        pl.semaphore_signal(barrier, inc=1, device_id=target, device_id_type=MESH)

    greet({"col": partner})
    greet({"row": x_near})
    greet({"row": y_near})

    @pl.when(is_end)
    def _():
        greet({"col": middle})
        greet({"row": far_corner})

    @pl.when(is_middle)
    def _():
        greet({"col": end})
        greet({"col": other_middle})

    own_a = pltpu.make_async_copy(a_in, a_all.at[col], local.at[0])
    own_b = pltpu.make_async_copy(b_in, b_all.at[row], local.at[1])
    own_a.start()
    own_b.start()
    pl.semaphore_wait(barrier, 5)

    @pl.when(is_end)
    def _():
        first = 2 * side + x
        second = 2 * side + 1 - x

        for step in range(PRE):
            a_copy(0, middle, col, step, True).start()

        @pl.when(donor)
        def _():
            @pl.loop(0, 2 * LENT)
            def _(step):
                c_copy(1, x, lent(step, True), True).start()
                c_copy(0, x, lent(step, False), True).start()

            @pl.loop(PRE, STEPS)
            def _(step):
                a_copy(0, middle, col, step, True).start()

        @pl.when(keeper)
        def _():
            @pl.loop(0, FINE)
            def _(step):
                b_copy(0, row, step, True).start()
                b_copy(1, row, step, True).start()

            for step in range(PRE, PRE + MORE):
                a_copy(0, middle, col, step, True).start()

        @pl.loop(0, STEPS)
        def _(step):
            a_copy(2, partner, col, step, True).start()
        out[...] = jnp.zeros_like(out)
        own_a.wait()
        own_b.wait()

        @pl.loop(0, LANDED_AT + STEPS)
        def _(t):
            @pl.when(keeper & (t < LENT))
            def _():
                for index in range(2):
                    chunk = lent(2 * t + index, True)
                    c_copy(0, 1 - x, chunk).wait_recv()
                    c_copy(0, 1 - x, chunk).start()

            @pl.when(keeper & (t == LENT))
            def _():
                @pl.loop(PRE + MORE, STEPS)
                def _(step):
                    a_copy(0, middle, col, step, True).start()

            @pl.when(keeper & (t == STEPS + 1))
            def _():
                b_wait(x_near, 0, FINE)

            @pl.when(donor & (t < STEPS))
            def _():
                for index in range(2):
                    b_copy(0, y_near, 2 * t + index).wait_recv()
                    b_copy(0, y_near, 2 * t + index).start()

            @pl.when(t < STEPS)
            def _():
                a_wait(middle, t)
                a_copy(2, partner, middle, t).start()
                a_wait(end + swap, t)

            @pl.when((t >= 1) & (t < STEPS + 1))
            def _():
                a_wait(middle + swap, t - 1)

            @pl.when(t == STEPS + 1)
            def _():
                split_b(first, 0, 8)

            @pl.when((t >= STEPS + 2) & (t < STEPS + 10))
            def _():
                u = t - STEPS - 2
                job(first, lax.div(u, GROUPS), lax.rem(u, GROUPS))

            @pl.when(donor & (t == STEPS + 12))
            def _():
                b_wait(far_corner, 0, FINE // 2)

            @pl.when(t == STEPS + 12)
            def _():
                split_b(second, 0, 4)

            @pl.when((t >= STEPS + 13) & (t < STEPS + 17))
            def _():
                job(second, 0, t - STEPS - 13)

            @pl.when(donor & (t == STEPS + 18))
            def _():
                b_wait(far_corner, FINE // 2, FINE)

            @pl.when(t == STEPS + 18)
            def _():
                split_b(second, 4, 8)

                @pl.loop(0, GROUPS)
                def _(index):
                    job(second, 1, index)

            @pl.when(t >= LANDED_AT)
            def _():
                part = rows_of(t - LANDED_AT, a_size)
                p_copy(t - LANDED_AT).wait_recv()
                out[part, :] += partial[part, :]

        @pl.when(donor)
        def _():
            c_sent(0, 2 * LENT * b_size)
            c_sent(1, 2 * LENT * b_size)
            b_sent(0, y_near, b_depth)

        @pl.when(keeper)
        def _():
            c_sent(0, 2 * LENT * b_size)
            b_sent(0, row, b_depth)
            b_sent(1, row, b_depth)
        a_sent(0, col)
        a_sent(2, col)
        a_sent(2, middle)

    @pl.when(is_middle)
    def _():
        inner = (row == 1) | (row == 2)
        slot = lax.rem(x + jnp.where(keeper, 1, 0), 2)
        mine = jnp.where(keeper, 2 * LACK, 0)
        theirs = 2 * LACK - mine

        def within(chunk, start):
            return (chunk >= start) & (chunk < start + 2 * LACK)

        def c_split(which, step):
            split_rows(which, rows_of(step, 2 * b_size), c_all, c_high, c_low)

        def c_landed(chunk):
            c_copy(0, 1 - slot, chunk).wait_recv()

            @pl.when(within(chunk, mine) & (lax.rem(chunk, 2) == 0))
            def _():
                c_copy(2, 1 - slot, chunk).start()

            @pl.when(within(chunk, theirs) & (lax.rem(chunk, 2) == 1))
            def _():
                c_copy(3, 1 - slot, chunk).start()

        @pl.loop(0, STEPS)
        def _(step):
            a_copy(0, other_middle, col, step, True).start()
            a_copy(1, end, col, step, True).start()

            @pl.when(step < HEAD)
            def _():
                b_copy(0, row, step, True).start()
                b_copy(1, row, step, True).start()
            a_copy(2, partner, col, step, True).start()
        out[...] = jnp.zeros_like(out)
        own_a.wait()
        own_b.wait()
        split_b(row, 0, 8)
        for step in range(PRE):
            a_wait(end, step)
            a_copy(0, other_middle, end, step).start()
            a_copy(2, partner, end, step).start()

        def sequence(s):
            def near(p):
                return jnp.where(p == 0, x_near, y_near)

            def choose(test, new, old):
                return tuple(jnp.where(test, a, b) for a, b in zip(new, old))

            u = lax.rem(s, 8)
            block, index = lax.div(u, GROUPS), lax.rem(u, GROUPS)
            value = choose(inner, (row, block, index), (near(block), 0, index))
            w = lax.rem(s, 2)
            g = jnp.where(s < 10, 0, jnp.where(s < 12, 1, jnp.where(s < 14, 0, jnp.where(s < 16, 1,
                jnp.where(s < 20, 2, 3)))))
            upper = ((s >= 12) & (s < 16)) | ((s >= 18) & (s < 20)) | (s >= 26)
            second = choose(inner, (near(w), 0, g), (row, w, g))
            second = choose(upper, (near(w), 1, g), second)
            value = choose(s >= 8, second, value)
            value = choose((s >= 20) & (s < 24), (far_corner, 0, s - 20), value)
            job(*value)

        def until(t):
            total = 0
            for when, count in ((17, 2), (18, 2), (19, 1), (20, 2), (21, 2), (22, 1), (24, 1), (25, 2),
                                (26, 2), (27, 1), (28, 2), (29, 2), (30, 2), (31, 1)):
                total = total + jnp.where(t >= when, count, 0)
            return total

        @pl.loop(0, SUM_AT + STEPS)
        def _(t):
            @pl.when(t < LENT)
            def _():
                for index in range(2):
                    chunk = lent(2 * t + index, keeper)
                    c_copy(0, slot, chunk).wait_recv()
                    both = within(chunk, theirs)

                    @pl.when(both | (lax.rem(chunk, 2) == 0))
                    def _():
                        c_copy(2, slot, chunk).start()

                    @pl.when(both | (lax.rem(chunk, 2) == 1))
                    def _():
                        c_copy(3, slot, chunk).start()
                c_split(slot, lax.div(lent(2 * t, keeper), 2))

            @pl.when(t < (FINE // 2 - HEAD) // 2)
            def _():
                for index in range(2):
                    b_copy(0, row, HEAD + 2 * t + index, True).start()
                    b_copy(1, row, HEAD + 2 * t + index, True).start()

            @pl.when(t < STEPS)
            def _():
                a_wait(other_middle, t)
                a_copy(2, partner, other_middle, t).start()

            @pl.when(t == OWN_AT)
            def _():
                @pl.loop(0, FINE // 2)
                def _(step):
                    b_copy(0, row, FINE // 2 + step, True).start()
                    b_copy(1, row, FINE // 2 + lax.rem(step + FINE // 4, FINE // 2), True).start()

            @pl.when(t == NEAR_AT)
            def _():
                b_wait(x_near, 0, FINE // 2)
                b_wait(y_near, 0, FINE // 2)

                @pl.loop(0, FINE // 4)
                def _(step):
                    b_copy(1, x_near, step).start()
                    b_copy(0, y_near, FINE // 4 + step).start()
                split_b(x_near, 0, 4)
                split_b(y_near, 0, 4)

            @pl.when(t == RELAY_AT)
            def _():
                b_wait(x_near, FINE // 2, FINE // 4 * 3)
                b_wait(y_near, FINE // 4 * 3, FINE)

                @pl.loop(0, FINE // 4)
                def _(step):
                    b_copy(1, x_near, FINE // 2 + step).start()
                    b_copy(0, y_near, FINE // 4 * 3 + step).start()

            @pl.when(t == LAST_AT)
            def _():
                b_wait(x_near, FINE // 4 * 3, FINE)
                b_wait(y_near, FINE // 2, FINE // 4 * 3)
                split_b(x_near, 4, 8)
                split_b(y_near, 4, 8)

            @pl.when(t == FAR_B_AT)
            def _():
                b_wait(far_corner, 0, FINE // 2)
                split_b(far_corner, 0, 4)

            @pl.when((t >= END_AT + PRE) & (t < END_AT + STEPS))
            def _():
                a_wait(end, t - END_AT)
                a_copy(0, other_middle, end, t - END_AT).start()
                a_copy(2, partner, end, t - END_AT).start()

            @pl.when((t >= FAR_AT) & (t < FAR_AT + STEPS))
            def _():
                a_wait(other_end, t - FAR_AT)
                a_copy(2, partner, other_end, t - FAR_AT).start()

            @pl.when((t >= 2) & (t < STEPS + 2))
            def _():
                a_wait(middle + swap, t - 2)
                a_wait(other_middle + swap, t - 2)

            @pl.when((t >= LENT_AT) & (t < LENT_AT + LENT))
            def _():
                u = t - LENT_AT

                @pl.when(u < LACK)
                def _():
                    c_landed(2 * u)
                    c_landed(2 * u + 1)
                    c_split(1 - slot, u)
                c_landed(2 * LACK + 2 * u)
                c_landed(2 * LACK + 2 * u + 1)
                c_split(1 - slot, LACK + u)

            @pl.when((t >= LACK_AT) & (t < LACK_AT + LACK))
            def _():
                chunk = mine + 2 * (t - LACK_AT)
                c_copy(0, slot, chunk).wait_recv()
                c_copy(0, slot, chunk + 1).wait_recv()
                c_split(slot, lax.div(chunk, 2))

            @pl.when((t > END_AT) & (t < END_AT + 1 + STEPS))
            def _():
                a_wait(end + swap, t - END_AT - 1)

            @pl.when((t == SUM_AT) | (t == SUM_AT + 3) | (t == SUM_AT + 7) | (t == SUM_AT + 11))
            def _():
                part = rows_of(lax.div(t - SUM_AT + 1, 4), group)
                partial[part, :] = (term(part, 2 * (2 - side), c_high, c_low, side, 0)
                                    + term(part, 2 * (2 - side) + 1, c_high, c_low, side, 1))

            @pl.when(t > SUM_AT)
            def _():
                @pl.loop(until(t - 1), until(t))
                def _(s):
                    sequence(s)

            @pl.when(t >= SUM_AT)
            def _():
                step = t - SUM_AT
                a_wait(other_end + swap, step)
                part = rows_of(step, a_size)
                partial[part, :] += (term(part, 6 - 6 * side, c_high, c_low, other_side, 0)
                                     + term(part, 7 - 6 * side, c_high, c_low, other_side, 1))
                p_copy(step).start()

        @pl.loop(until(SUM_AT + STEPS), 7 * GROUPS)
        def _(s):
            sequence(s)

        b_wait(far_corner, FINE // 2, FINE)
        split_b(far_corner, 4, 8)

        @pl.loop(0, 2)
        def _(index):
            job(far_corner, 1, index, 2 * group)

        for kind in range(3):
            a_sent(kind, col)
        a_sent(2, other_middle)
        a_sent(0, end)
        a_sent(2, end)
        a_sent(2, other_end)
        c_sent(2, (FINE // 2 + LACK) * b_size)
        c_sent(3, (FINE // 2 + LACK) * b_size)
        b_sent(0, row, b_depth)
        b_sent(1, row, b_depth)
        b_sent(0, y_near, b_depth // 2)
        b_sent(1, x_near, b_depth // 2)
        remote(partial, partial, p_send, p_recv.at[0], {"col": end}).wait_send()


def shared_body(left_matrix, right_matrix):
    height, a_depth = left_matrix.shape
    b_depth, width = right_matrix.shape
    dma = pltpu.SemaphoreType.DMA
    return pl.pallas_call(
        shared_kernel,
        out_shape=jax.ShapeDtypeStruct((height, width), jnp.float32),
        in_specs=[pl.BlockSpec(memory_space=pltpu.HBM)] * 2,
        out_specs=pl.BlockSpec(memory_space=pltpu.VMEM),
        scratch_shapes=[
            pltpu.VMEM((8, height, a_depth), jnp.float32),
            pltpu.VMEM((4, b_depth, width), jnp.float32),
            pltpu.VMEM((4, b_depth, width), jnp.bfloat16),
            pltpu.VMEM((4, b_depth, width), jnp.bfloat16),
            pltpu.VMEM((2, b_depth, width), jnp.float32),
            pltpu.VMEM((2, b_depth, width), jnp.bfloat16),
            pltpu.VMEM((2, b_depth, width), jnp.bfloat16),
            pltpu.VMEM((height, width), jnp.float32),
            dma((8, STEPS)), dma((3, 8)), dma((4, FINE)), dma((2, 4)),
            dma((2, FINE)), dma((4,)), dma((STEPS,)), dma(()), dma((2,)),
        ],
        compiler_params=pltpu.CompilerParams(
            collective_id=1, has_side_effects=True, vmem_limit_bytes=48 * 2**20),
    )(left_matrix, right_matrix)


def solution(mesh):
    placed = (P("row", "col"), P("row", "col"))
    rows, cols = mesh.shape["row"], mesh.shape["col"]
    part = shared_body if (rows, cols) == (4, 8) else functools.partial(body, rows, cols)
    return jax.shard_map(
        part, mesh=mesh, in_specs=placed, out_specs=P("row", "col"), check_vma=False
    )
```

```python
import functools

import jax
import jax.numpy as jnp
from jax import lax
from jax.experimental import pallas as pl
from jax.experimental.pallas import tpu as pltpu
from jax.sharding import PartitionSpec as P

MESH = pl.DeviceIdType.MESH
CHUNKS = 4


def split(value):
    high = value.astype(jnp.bfloat16)
    low = (value - high.astype(jnp.float32)).astype(jnp.bfloat16)
    return high, low


def kernel(rows, cols, a_in, b_in, out, a_all, b_all, b_high, b_low,
           a_recv, a_send, b_recv, b_send, local):
    row = lax.axis_index("row")
    col = lax.axis_index("col")
    core = lax.rem(col, 2)
    chip = lax.div(col, 2)
    chips = cols // 2
    height, a_depth = a_in.shape
    b_depth = b_in.shape[0]
    per_b = b_depth // a_depth
    size = height // CHUNKS
    partner = chip * 2 + 1 - core

    def left_valid(distance):
        return chip >= distance

    def right_valid(distance):
        return chip + distance < chips

    def a_copy(kind, block, chunk, own):
        part = pl.ds(chunk * size, size)
        target = (col + 2, col - 2, partner)[kind]
        return pltpu.make_async_remote_copy(
            src_ref=a_in.at[part] if own else a_all.at[block, part],
            dst_ref=a_all.at[block, part],
            send_sem=a_send.at[kind, block, chunk],
            recv_sem=a_recv.at[block, chunk],
            device_id={"col": target}, device_id_type=MESH)

    def a_wait(block, chunk):
        a_copy(2, block, chunk, False).wait_recv()

    def b_copy(peer, source):
        return pltpu.make_async_remote_copy(
            src_ref=b_in, dst_ref=b_all.at[source],
            send_sem=b_send.at[peer], recv_sem=b_recv.at[source],
            device_id={"row": peer}, device_id_type=MESH)

    barrier = pltpu.get_barrier_semaphore()

    @pl.when(chip > 0)
    def _():
        pl.semaphore_signal(barrier, inc=1, device_id={"col": col - 2}, device_id_type=MESH)

    @pl.when(chip < chips - 1)
    def _():
        pl.semaphore_signal(barrier, inc=1, device_id={"col": col + 2}, device_id_type=MESH)

    pl.semaphore_signal(barrier, inc=1, device_id={"col": partner}, device_id_type=MESH)
    peers = [lax.rem(row + offset, rows) for offset in range(1, rows)]
    for peer in peers:
        pl.semaphore_signal(barrier, inc=1, device_id={"row": peer}, device_id_type=MESH)
    own_a = pltpu.make_async_copy(a_in, a_all.at[col], local.at[0])
    own_b = pltpu.make_async_copy(b_in, b_all.at[row], local.at[1])
    own_a.start()
    own_b.start()
    near = jnp.where(chip > 0, 1, 0) + jnp.where(chip < chips - 1, 1, 0)
    pl.semaphore_wait(barrier, rows + near)

    for chunk in range(CHUNKS):
        @pl.when(right_valid(1))
        def _():
            a_copy(0, col, chunk, True).start()

        @pl.when(left_valid(1))
        def _():
            a_copy(1, col, chunk, True).start()
    for peer in peers:
        b_copy(peer, row).start()
    for chunk in range(CHUNKS):
        a_copy(2, col, chunk, True).start()

    out[...] = jnp.zeros_like(out)
    own_a.wait()
    own_b.wait()

    def multiply(block, chunk):
        part = pl.ds(pl.multiple_of(chunk * size, size), size)
        source = lax.div(block, per_b)
        offset = pl.multiple_of(lax.rem(block, per_b) * a_depth, a_depth)
        depth = pl.ds(offset, a_depth)
        high, low = split(a_all[block, part, :])
        right_high = b_high[source, depth, :]
        right_low = b_low[source, depth, :]
        dot = functools.partial(jnp.dot, preferred_element_type=jnp.float32)
        out[part, :] += (dot(low, right_high) + dot(high, right_low)) + dot(high, right_high)

    def split_b(source):
        @pl.loop(0, b_depth // 128)
        def _(index):
            part = pl.ds(pl.multiple_of(index * 128, 128), 128)
            high, low = split(b_all[source, part, :])
            b_high[source, part, :] = high
            b_low[source, part, :] = low

    def multiply_block(block):
        @pl.loop(0, CHUNKS)
        def _(chunk):
            multiply(block, chunk)

    for distance in range(1, chips - 1):
        for chunk in range(CHUNKS):
            @pl.when(left_valid(distance))
            def _():
                block = col - 2 * distance
                a_wait(block, chunk)

                @pl.when(right_valid(1))
                def _():
                    a_copy(0, block, chunk, False).start()
                a_copy(2, block, chunk, False).start()

            @pl.when(right_valid(distance))
            def _():
                block = col + 2 * distance
                a_wait(block, chunk)

                @pl.when(left_valid(1))
                def _():
                    a_copy(1, block, chunk, False).start()
                a_copy(2, block, chunk, False).start()

    split_b(row)
    for peer in peers:
        b_copy(peer, peer).wait_recv()
        split_b(peer)

    for chunk in range(CHUNKS):
        a_wait(partner, chunk)
    multiply_block(col)
    multiply_block(partner)
    for distance in range(1, chips - 1):
        for valid, step in ((left_valid, -2), (right_valid, 2)):
            @pl.when(valid(distance))
            def _():
                for chunk in range(CHUNKS):
                    a_wait(partner + step * distance, chunk)
                multiply_block(col + step * distance)
                multiply_block(partner + step * distance)

    if chips > 1:
        for valid, step in ((left_valid, -2), (right_valid, 2)):
            @pl.when(valid(chips - 1))
            def _():
                block = col + step * (chips - 1)
                other = partner + step * (chips - 1)
                for chunk in range(CHUNKS):
                    a_wait(block, chunk)
                    a_copy(2, block, chunk, False).start()
                    multiply(block, chunk)
                    a_wait(other, chunk)
                    multiply(other, chunk)

    for peer in peers:
        b_copy(peer, row).wait_send()
    for chunk in range(CHUNKS):
        a_copy(2, col, chunk, True).wait_send()
        for distance in range(0, chips):
            @pl.when(left_valid(distance) & right_valid(1))
            def _():
                a_copy(0, col - 2 * distance, chunk, False).wait_send()

            @pl.when(right_valid(distance) & left_valid(1))
            def _():
                a_copy(1, col + 2 * distance, chunk, False).wait_send()
        for distance in range(1, chips):
            @pl.when(left_valid(distance))
            def _():
                a_copy(2, col - 2 * distance, chunk, False).wait_send()

            @pl.when(right_valid(distance))
            def _():
                a_copy(2, col + 2 * distance, chunk, False).wait_send()


def body(rows, cols, left_matrix, right_matrix):
    height, a_depth = left_matrix.shape
    b_depth, width = right_matrix.shape
    return pl.pallas_call(
        functools.partial(kernel, rows, cols),
        out_shape=jax.ShapeDtypeStruct((height, width), jnp.float32),
        in_specs=[pl.BlockSpec(memory_space=pltpu.HBM)] * 2,
        out_specs=pl.BlockSpec(memory_space=pltpu.VMEM),
        scratch_shapes=[
            pltpu.VMEM((cols, height, a_depth), jnp.float32),
            pltpu.VMEM((rows, b_depth, width), jnp.float32),
            pltpu.VMEM((rows, b_depth, width), jnp.bfloat16),
            pltpu.VMEM((rows, b_depth, width), jnp.bfloat16),
            pltpu.SemaphoreType.DMA((cols, CHUNKS)),
            pltpu.SemaphoreType.DMA((3, cols, CHUNKS)),
            pltpu.SemaphoreType.DMA((rows,)),
            pltpu.SemaphoreType.DMA((rows,)),
            pltpu.SemaphoreType.DMA((2,)),
        ],
        compiler_params=pltpu.CompilerParams(
            collective_id=0, has_side_effects=True, vmem_limit_bytes=56 * 2**20),
    )(left_matrix, right_matrix)


STEPS = 16
FINE = 32
HEAD = 8
PRE = 1
MORE = 1
GROUPS = 4
LACK = 2
LENT = FINE // 2 - LACK
LENT_AT = 3
LACK_AT = 5
OWN_AT = 14
NEAR_AT = 16
RELAY_AT = 21
LAST_AT = 24
FAR_B_AT = 28
END_AT = 14
FAR_AT = 16
SUM_AT = 16
LANDED_AT = 20


def shared_kernel(a_in, b_in, out, a_all, b_all, b_high, b_low, c_all, c_high, c_low, partial,
                  a_recv, a_send, b_recv, b_send, c_recv, c_send, p_recv, p_send, local):
    row = lax.axis_index("row")
    col = lax.axis_index("col")
    core = lax.rem(col, 2)
    chip = lax.div(col, 2)
    partner = chip * 2 + 1 - core
    side = lax.div(chip, 2)
    y = lax.div(row, 2)
    x = lax.rem(row, 2)
    x_near = y * 2 + 1 - x
    y_near = (1 - y) * 2 + x
    far_corner = (1 - y) * 2 + 1 - x
    other_side = 1 - side
    end = 6 * side + core
    middle = 2 + 2 * side + core
    other_middle = 4 - 2 * side + core
    other_end = 6 - 6 * side + core
    swap = 1 - 2 * core
    is_end = (chip == 0) | (chip == 3)
    is_middle = (chip == 1) | (chip == 2)
    keeper = y == side
    donor = y == other_side
    height, a_depth = a_in.shape
    b_depth = b_in.shape[0]
    a_size = height // STEPS
    b_size = b_depth // FINE
    group = height // GROUPS

    def rows_of(index, size):
        return pl.ds(pl.multiple_of(index * size, size), size)

    def remote(source, target, send, recv, device):
        return pltpu.make_async_remote_copy(
            src_ref=source, dst_ref=target, send_sem=send, recv_sem=recv,
            device_id=device, device_id_type=MESH)

    def a_copy(kind, target, block, step, own=False):
        part = rows_of(step, a_size)
        return remote(a_in.at[part] if own else a_all.at[block, part], a_all.at[block, part],
                      a_send.at[kind, block], a_recv.at[block, step], {"col": target})

    def a_wait(block, step):
        a_copy(2, partner, block, step).wait_recv()

    def a_sent(kind, block):
        remote(a_all.at[block], a_all.at[block], a_send.at[kind, block], a_recv.at[block, 0],
               {"col": partner}).wait_send()

    def b_copy(kind, source, step, own=False):
        part = rows_of(step, b_size)
        return remote(b_in.at[part] if own else b_all.at[source, part], b_all.at[source, part],
                      b_send.at[kind, source], b_recv.at[source, step],
                      {"row": (x_near, y_near)[kind]})

    def b_wait(source, first, last):
        @pl.loop(first, last)
        def _(step):
            b_copy(0, source, step).wait_recv()

    def b_sent(kind, source, size):
        part = pl.ds(0, size)
        remote(b_all.at[source, part], b_all.at[source, part], b_send.at[kind, source],
               b_recv.at[source, 0], {"row": x_near}).wait_send()

    def c_copy(kind, slot, step, own=False):
        part = rows_of(step, b_size)
        target = ({"col": middle}, {"row": far_corner}, {"row": x_near}, {"row": y_near})[kind]
        return remote(b_in.at[part] if own else c_all.at[slot, part], c_all.at[slot, part],
                      c_send.at[kind], c_recv.at[slot, step], target)

    def c_sent(kind, size):
        part = pl.ds(0, size)
        remote(c_all.at[0, part], c_all.at[0, part], c_send.at[kind], c_recv.at[0, 0],
               {"row": x_near}).wait_send()

    def lent(step, held):
        return step + jnp.where(held & (step < 2 * LACK), 0, 2 * LACK)

    def p_copy(step):
        part = rows_of(step, a_size)
        return remote(partial.at[part], partial.at[part], p_send, p_recv.at[step], {"col": end})

    def split_rows(source, part, full, high_all, low_all):
        high, low = split(full[source, part, :])
        high_all[source, part, :] = high
        low_all[source, part, :] = low

    def split_b(source, first, last):
        @pl.loop(first, last)
        def _(index):
            split_rows(source, rows_of(index, 4 * b_size), b_all, b_high, b_low)

    dot = functools.partial(jnp.dot, preferred_element_type=jnp.float32)

    def term(part, block, high_all, low_all, source, half):
        depth = rows_of(half, a_depth)
        high, low = split(a_all[block, part, :])
        right_high = high_all[source, depth, :]
        right_low = low_all[source, depth, :]
        return (dot(low, right_high) + dot(high, right_low)) + dot(high, right_high)

    def job(source, half, index, size=group):
        part = rows_of(index, size)
        out[part, :] += term(part, 2 * source + half, b_high, b_low, source, half)

    barrier = pltpu.get_barrier_semaphore()

    def greet(target):
        pl.semaphore_signal(barrier, inc=1, device_id=target, device_id_type=MESH)

    greet({"col": partner})
    greet({"row": x_near})
    greet({"row": y_near})

    @pl.when(is_end)
    def _():
        greet({"col": middle})
        greet({"row": far_corner})

    @pl.when(is_middle)
    def _():
        greet({"col": end})
        greet({"col": other_middle})

    own_a = pltpu.make_async_copy(a_in, a_all.at[col], local.at[0])
    own_b = pltpu.make_async_copy(b_in, b_all.at[row], local.at[1])
    own_a.start()
    own_b.start()
    pl.semaphore_wait(barrier, 5)

    @pl.when(is_end)
    def _():
        first = 2 * side + x
        second = 2 * side + 1 - x

        for step in range(PRE):
            a_copy(0, middle, col, step, True).start()

        @pl.when(donor)
        def _():
            @pl.loop(0, 2 * LENT)
            def _(step):
                c_copy(1, x, lent(step, True), True).start()
                c_copy(0, x, lent(step, False), True).start()

            @pl.loop(PRE, STEPS)
            def _(step):
                a_copy(0, middle, col, step, True).start()

        @pl.when(keeper)
        def _():
            @pl.loop(0, FINE)
            def _(step):
                b_copy(0, row, step, True).start()
                b_copy(1, row, step, True).start()

            for step in range(PRE, PRE + MORE):
                a_copy(0, middle, col, step, True).start()

        @pl.loop(0, STEPS)
        def _(step):
            a_copy(2, partner, col, step, True).start()
        out[...] = jnp.zeros_like(out)
        own_a.wait()
        own_b.wait()

        @pl.loop(0, LANDED_AT + STEPS)
        def _(t):
            @pl.when(keeper & (t < LENT))
            def _():
                for index in range(2):
                    chunk = lent(2 * t + index, True)
                    c_copy(0, 1 - x, chunk).wait_recv()
                    c_copy(0, 1 - x, chunk).start()

            @pl.when(keeper & (t == LENT))
            def _():
                @pl.loop(PRE + MORE, STEPS)
                def _(step):
                    a_copy(0, middle, col, step, True).start()

            @pl.when(keeper & (t == STEPS + 1))
            def _():
                b_wait(x_near, 0, FINE)

            @pl.when(donor & (t < STEPS))
            def _():
                for index in range(2):
                    b_copy(0, y_near, 2 * t + index).wait_recv()
                    b_copy(0, y_near, 2 * t + index).start()

            @pl.when(t < STEPS)
            def _():
                a_wait(middle, t)
                a_copy(2, partner, middle, t).start()
                a_wait(end + swap, t)

            @pl.when((t >= 1) & (t < STEPS + 1))
            def _():
                a_wait(middle + swap, t - 1)

            @pl.when(t == STEPS + 1)
            def _():
                split_b(first, 0, 8)

            @pl.when((t >= STEPS + 2) & (t < STEPS + 10))
            def _():
                u = t - STEPS - 2
                job(first, lax.div(u, GROUPS), lax.rem(u, GROUPS))

            @pl.when(donor & (t == STEPS + 12))
            def _():
                b_wait(far_corner, 0, FINE // 2)

            @pl.when(t == STEPS + 12)
            def _():
                split_b(second, 0, 4)

            @pl.when((t >= STEPS + 13) & (t < STEPS + 17))
            def _():
                job(second, 0, t - STEPS - 13)

            @pl.when(donor & (t == STEPS + 18))
            def _():
                b_wait(far_corner, FINE // 2, FINE)

            @pl.when(t == STEPS + 18)
            def _():
                split_b(second, 4, 8)

                @pl.loop(0, GROUPS)
                def _(index):
                    job(second, 1, index)

            @pl.when(t >= LANDED_AT)
            def _():
                part = rows_of(t - LANDED_AT, a_size)
                p_copy(t - LANDED_AT).wait_recv()
                out[part, :] += partial[part, :]

        @pl.when(donor)
        def _():
            c_sent(0, 2 * LENT * b_size)
            c_sent(1, 2 * LENT * b_size)
            b_sent(0, y_near, b_depth)

        @pl.when(keeper)
        def _():
            c_sent(0, 2 * LENT * b_size)
            b_sent(0, row, b_depth)
            b_sent(1, row, b_depth)
        a_sent(0, col)
        a_sent(2, col)
        a_sent(2, middle)

    @pl.when(is_middle)
    def _():
        inner = (row == 1) | (row == 2)
        slot = lax.rem(x + jnp.where(keeper, 1, 0), 2)
        mine = jnp.where(keeper, 2 * LACK, 0)
        theirs = 2 * LACK - mine

        def within(chunk, start):
            return (chunk >= start) & (chunk < start + 2 * LACK)

        def c_split(which, step):
            split_rows(which, rows_of(step, 2 * b_size), c_all, c_high, c_low)

        def c_landed(chunk):
            c_copy(0, 1 - slot, chunk).wait_recv()

            @pl.when(within(chunk, mine) & (lax.rem(chunk, 2) == 0))
            def _():
                c_copy(2, 1 - slot, chunk).start()

            @pl.when(within(chunk, theirs) & (lax.rem(chunk, 2) == 1))
            def _():
                c_copy(3, 1 - slot, chunk).start()

        @pl.loop(0, STEPS)
        def _(step):
            a_copy(0, other_middle, col, step, True).start()
            a_copy(1, end, col, step, True).start()

            @pl.when(step < HEAD)
            def _():
                b_copy(0, row, step, True).start()
                b_copy(1, row, step, True).start()
            a_copy(2, partner, col, step, True).start()
        out[...] = jnp.zeros_like(out)
        own_a.wait()
        own_b.wait()
        split_b(row, 0, 8)
        for step in range(PRE):
            a_wait(end, step)
            a_copy(0, other_middle, end, step).start()
            a_copy(2, partner, end, step).start()

        def sequence(s):
            def near(p):
                return jnp.where(p == 0, x_near, y_near)

            def choose(test, new, old):
                return tuple(jnp.where(test, a, b) for a, b in zip(new, old))

            u = lax.rem(s, 8)
            block, index = lax.div(u, GROUPS), lax.rem(u, GROUPS)
            value = choose(inner, (row, block, index), (near(block), 0, index))
            w = lax.rem(s, 2)
            g = jnp.where(s < 10, 0, jnp.where(s < 12, 1, jnp.where(s < 14, 0, jnp.where(s < 16, 1,
                jnp.where(s < 20, 2, 3)))))
            upper = ((s >= 12) & (s < 16)) | ((s >= 18) & (s < 20)) | (s >= 26)
            second = choose(inner, (near(w), 0, g), (row, w, g))
            second = choose(upper, (near(w), 1, g), second)
            value = choose(s >= 8, second, value)
            value = choose((s >= 20) & (s < 24), (far_corner, 0, s - 20), value)
            job(*value)

        def until(t):
            total = 0
            for when, count in ((17, 2), (18, 2), (19, 1), (20, 2), (21, 2), (22, 1), (24, 1), (25, 2),
                                (26, 2), (27, 1), (28, 2), (29, 2), (30, 2), (31, 1)):
                total = total + jnp.where(t >= when, count, 0)
            return total

        @pl.loop(0, SUM_AT + STEPS)
        def _(t):
            @pl.when(t < LENT)
            def _():
                for index in range(2):
                    chunk = lent(2 * t + index, keeper)
                    c_copy(0, slot, chunk).wait_recv()
                    both = within(chunk, theirs)

                    @pl.when(both | (lax.rem(chunk, 2) == 0))
                    def _():
                        c_copy(2, slot, chunk).start()

                    @pl.when(both | (lax.rem(chunk, 2) == 1))
                    def _():
                        c_copy(3, slot, chunk).start()
                c_split(slot, lax.div(lent(2 * t, keeper), 2))

            @pl.when(t < (FINE // 2 - HEAD) // 2)
            def _():
                for index in range(2):
                    b_copy(0, row, HEAD + 2 * t + index, True).start()
                    b_copy(1, row, HEAD + 2 * t + index, True).start()

            @pl.when(t < STEPS)
            def _():
                a_wait(other_middle, t)
                a_copy(2, partner, other_middle, t).start()

            @pl.when(t == OWN_AT)
            def _():
                @pl.loop(0, FINE // 2)
                def _(step):
                    b_copy(0, row, FINE // 2 + step, True).start()
                    b_copy(1, row, FINE // 2 + lax.rem(step + FINE // 4, FINE // 2), True).start()

            @pl.when(t == NEAR_AT)
            def _():
                b_wait(x_near, 0, FINE // 2)
                b_wait(y_near, 0, FINE // 2)

                @pl.loop(0, FINE // 4)
                def _(step):
                    b_copy(1, x_near, step).start()
                    b_copy(0, y_near, FINE // 4 + step).start()
                split_b(x_near, 0, 4)
                split_b(y_near, 0, 4)

            @pl.when(t == RELAY_AT)
            def _():
                b_wait(x_near, FINE // 2, FINE // 4 * 3)
                b_wait(y_near, FINE // 4 * 3, FINE)

                @pl.loop(0, FINE // 4)
                def _(step):
                    b_copy(1, x_near, FINE // 2 + step).start()
                    b_copy(0, y_near, FINE // 4 * 3 + step).start()

            @pl.when(t == LAST_AT)
            def _():
                b_wait(x_near, FINE // 4 * 3, FINE)
                b_wait(y_near, FINE // 2, FINE // 4 * 3)
                split_b(x_near, 4, 8)
                split_b(y_near, 4, 8)

            @pl.when(t == FAR_B_AT)
            def _():
                b_wait(far_corner, 0, FINE // 2)
                split_b(far_corner, 0, 4)

            @pl.when((t >= END_AT + PRE) & (t < END_AT + STEPS))
            def _():
                a_wait(end, t - END_AT)
                a_copy(0, other_middle, end, t - END_AT).start()
                a_copy(2, partner, end, t - END_AT).start()

            @pl.when((t >= FAR_AT) & (t < FAR_AT + STEPS))
            def _():
                a_wait(other_end, t - FAR_AT)
                a_copy(2, partner, other_end, t - FAR_AT).start()

            @pl.when((t >= 2) & (t < STEPS + 2))
            def _():
                a_wait(middle + swap, t - 2)
                a_wait(other_middle + swap, t - 2)

            @pl.when((t >= LENT_AT) & (t < LENT_AT + LENT))
            def _():
                u = t - LENT_AT

                @pl.when(u < LACK)
                def _():
                    c_landed(2 * u)
                    c_landed(2 * u + 1)
                    c_split(1 - slot, u)
                c_landed(2 * LACK + 2 * u)
                c_landed(2 * LACK + 2 * u + 1)
                c_split(1 - slot, LACK + u)

            @pl.when((t >= LACK_AT) & (t < LACK_AT + LACK))
            def _():
                chunk = mine + 2 * (t - LACK_AT)
                c_copy(0, slot, chunk).wait_recv()
                c_copy(0, slot, chunk + 1).wait_recv()
                c_split(slot, lax.div(chunk, 2))

            @pl.when((t > END_AT) & (t < END_AT + 1 + STEPS))
            def _():
                a_wait(end + swap, t - END_AT - 1)

            @pl.when((t == SUM_AT) | (t == SUM_AT + 3) | (t == SUM_AT + 7) | (t == SUM_AT + 11))
            def _():
                part = rows_of(lax.div(t - SUM_AT + 1, 4), group)
                partial[part, :] = (term(part, 2 * (2 - side), c_high, c_low, side, 0)
                                    + term(part, 2 * (2 - side) + 1, c_high, c_low, side, 1))

            @pl.when(t > SUM_AT)
            def _():
                @pl.loop(until(t - 1), until(t))
                def _(s):
                    sequence(s)

            @pl.when(t >= SUM_AT)
            def _():
                step = t - SUM_AT
                a_wait(other_end + swap, step)
                part = rows_of(step, a_size)
                partial[part, :] += (term(part, 6 - 6 * side, c_high, c_low, other_side, 0)
                                     + term(part, 7 - 6 * side, c_high, c_low, other_side, 1))
                p_copy(step).start()

        @pl.loop(until(SUM_AT + STEPS), 7 * GROUPS)
        def _(s):
            sequence(s)

        b_wait(far_corner, FINE // 2, FINE)
        split_b(far_corner, 4, 8)

        @pl.loop(0, 2)
        def _(index):
            job(far_corner, 1, index, 2 * group)

        for kind in range(3):
            a_sent(kind, col)
        a_sent(2, other_middle)
        a_sent(0, end)
        a_sent(2, end)
        a_sent(2, other_end)
        c_sent(2, (FINE // 2 + LACK) * b_size)
        c_sent(3, (FINE // 2 + LACK) * b_size)
        b_sent(0, row, b_depth)
        b_sent(1, row, b_depth)
        b_sent(0, y_near, b_depth // 2)
        b_sent(1, x_near, b_depth // 2)
        remote(partial, partial, p_send, p_recv.at[0], {"col": end}).wait_send()


def shared_body(left_matrix, right_matrix):
    height, a_depth = left_matrix.shape
    b_depth, width = right_matrix.shape
    dma = pltpu.SemaphoreType.DMA
    return pl.pallas_call(
        shared_kernel,
        out_shape=jax.ShapeDtypeStruct((height, width), jnp.float32),
        in_specs=[pl.BlockSpec(memory_space=pltpu.HBM)] * 2,
        out_specs=pl.BlockSpec(memory_space=pltpu.VMEM),
        scratch_shapes=[
            pltpu.VMEM((8, height, a_depth), jnp.float32),
            pltpu.VMEM((4, b_depth, width), jnp.float32),
            pltpu.VMEM((4, b_depth, width), jnp.bfloat16),
            pltpu.VMEM((4, b_depth, width), jnp.bfloat16),
            pltpu.VMEM((2, b_depth, width), jnp.float32),
            pltpu.VMEM((2, b_depth, width), jnp.bfloat16),
            pltpu.VMEM((2, b_depth, width), jnp.bfloat16),
            pltpu.VMEM((height, width), jnp.float32),
            dma((8, STEPS)), dma((3, 8)), dma((4, FINE)), dma((2, 4)),
            dma((2, FINE)), dma((4,)), dma((STEPS,)), dma(()), dma((2,)),
        ],
        compiler_params=pltpu.CompilerParams(
            collective_id=1, has_side_effects=True, vmem_limit_bytes=48 * 2**20),
    )(left_matrix, right_matrix)


def solution(mesh):
    placed = (P("row", "col"), P("row", "col"))
    rows, cols = mesh.shape["row"], mesh.shape["col"]
    part = shared_body if (rows, cols) == (4, 8) else functools.partial(body, rows, cols)
    return jax.shard_map(
        part, mesh=mesh, in_specs=placed, out_specs=P("row", "col"), check_vma=False
    )
```
